32 devices in a mesh: leaf: 16 (over z, y, x), player: 2 (over core).
Axes of the slice: x: 2, y: 2, z: 4, core: 2. Of those that a mesh axis runs over, the one named last changes fastest.
Arguments:
- chance_reach: float32 [2, 512, 1326], P('player', 'leaf'), may hold values from 0.02 to 1
- regrets_start: float32 [2, 512, 1326], P('player', 'leaf'), may hold values from -6 to 6
- pot: float32 [512], P('leaf'), may hold values from 1 to 8
- parent: int32 [2, 512], P('player'), may hold values from 0 to 255, never falling along the last dimension, each value on 1 to 6 neighbouring positions
- hand_cards: int32 [1326, 2], replicated, may hold values from 0 to 51, as said below
- board_cards: int32 [64, 5], P('leaf'), may hold values from 0 to 51, as said below
- hand_rank: int32 [64, 1326], P('leaf'), may hold values from 0 to 1999
Outputs:
- regrets: float32 [2, 512, 1326], P('player', 'leaf')
- values: float32 [2, 512, 1326], P('player', 'leaf')
The draws below stay inside these ranges and needn't reach their ends.
Inputs may be any that keep to these rules, and one draw needn't show every extreme that they name: `parent`: along each row the node ids never fall; each node owns 1 to 6 consecutive leaves, one exactly 6; every id up to 255 occurs. `hand_cards`: distinct pairs of two different cards, the smaller card first. `board_cards`: five different cards on each board.
All inputs are finite; a program needn't handle non-finite values.
Results may differ from the reference program's by a relative error of at most 0.0003.
Values sent between devices are 32-bit elements; how exact they have to be, the bound alone decides.
A program may use at most 128 MiB of HBM per device.

```python
import math
import jax
import jax.numpy as jnp
import numpy as np
from jax import lax

H = 1326
BOARD_LEAVES = 8
MOST = 6
ITERS = 2
LEAVES = 512
BOARDS = 64
NODES = 256


def draw_hand_cards(key, part):
    lower_cards, upper_cards = np.triu_indices(52, 1)
    card_pairs = jnp.stack([jnp.asarray(lower_cards, jnp.int32), jnp.asarray(upper_cards, jnp.int32)], axis=1)
    chosen = jax.random.permutation(jax.random.fold_in(key, 3), card_pairs.shape[0])[:H]
    return card_pairs[chosen].astype(jnp.int32)


def draw_board_cards(key, part):
    board_keys = jax.random.split(jax.random.fold_in(key, 7), BOARDS)
    return jax.vmap(lambda board_key: jax.random.permutation(board_key, 52)[:5])(board_keys).astype(jnp.int32)


def place_ends(values, rng, least, high):
    longest = values.shape.index(max(values.shape))
    spots = []
    for shift in (0, 1):
        where = [jax.random.randint(jax.random.fold_in(rng, axis), (), 0, length) for axis, length in enumerate(values.shape)]
        where[longest] = (where[longest] + shift) % values.shape[longest]
        spots.append(tuple(where))
    return values.at[spots[0]].set(least).at[spots[1]].set(high)


def levels(rng, shape, cuts, least, top_value):
    factor_of, own = 1.0, jax.random.fold_in(rng, 6)
    for axis_at, blocks in cuts:
        draws = jnp.exp(jax.random.uniform(jax.random.fold_in(own, axis_at), (blocks,), jnp.float32, least / len(cuts), top_value / len(cuts)))
        factor_of = factor_of * jnp.repeat(draws, shape[axis_at] // blocks).reshape([-1 if axis == axis_at else 1 for axis in range(len(shape))])
    return factor_of


def profile(amount, total, limit, skew):
    portions = [(1 << 20) // math.isqrt(standing ** skew) + 1 for standing in range(2, amount + 1)]
    surplus, given = total - limit - (amount - 1), [1] * (amount - 1)
    while surplus > 0:
        movable = [i for i in range(amount - 1) if given[i] < limit]
        mass, budget = sum([portions[i] for i in movable]), surplus
        for i in movable:
            extra = min(limit - given[i], max(1, budget * portions[i] // mass), surplus)
            given[i] = given[i] + extra
            surplus = surplus - extra
    return np.array([limit] + given)


def ragged(key, number_of, total, most, slope):
    if number_of == 2:
        one = jax.random.randint(key, (), max(1, total - most), min(most, total - 1) + 1)
        return jnp.stack([one, total - one])
    lengths = jnp.asarray(profile(number_of, total, most, slope), jnp.int32)
    couples = (number_of - 1) // 2
    source_of, sink = lengths[1:1 + 2 * couples:2], lengths[2:2 + 2 * couples:2]
    room = jnp.minimum(source_of - 1, most - sink)
    shifted = jax.random.randint(jax.random.fold_in(key, 1), (couples,), 0, 1 << 20) % (room + 1)
    lengths = lengths.at[1:1 + 2 * couples:2].set(source_of - shifted).at[2:2 + 2 * couples:2].set(sink + shifted)
    return lengths[jax.random.permutation(jax.random.fold_in(key, 2), number_of)]


def bell_draw(rng, shape, width, bound, cuts=(), kind=jnp.bfloat16):
    factor_of = levels(rng, shape, cuts, -0.22, 0.18) if cuts else 1.0
    values = jax.random.normal(rng, shape, jnp.float32) * width * factor_of
    return jnp.minimum(jnp.maximum(values, -bound), bound).astype(kind)


def setup_inputs(seed: int = 0) -> dict:
    arg_keys = jax.random.split(jax.random.key(seed), 8)
    return {
        "chance_reach": jnp.clip(jnp.exp(math.log(1.0) - 3.912023 * jax.random.uniform(arg_keys[0], (2, LEAVES, H), jnp.float32) ** levels(arg_keys[0], (2, LEAVES, H), ((0, 2), (1, 16)), -0.2, 0.2)), 0.02, 1.0),
        "regrets_start": bell_draw(arg_keys[1], (2, LEAVES, H), 1.0, 6.0, ((0, 2), (1, 16)), jnp.float32),
        "pot": jnp.clip(jnp.exp(math.log(8.0) - 2.0794415 * jax.random.uniform(arg_keys[2], (LEAVES,), jnp.float32) ** levels(arg_keys[2], (LEAVES,), ((0, 16),), -0.2, 0.2)), 1.0, 8.0),
        "parent": jax.vmap(lambda own: jnp.searchsorted(jnp.cumsum(ragged(own, NODES, LEAVES, MOST, 2)), jnp.arange(LEAVES), side="right"))(jax.random.split(arg_keys[3], 2)).reshape((2, LEAVES)).astype(jnp.int32),
        "hand_cards": draw_hand_cards(jax.random.fold_in(arg_keys[7], 71), 0),
        "board_cards": draw_board_cards(jax.random.fold_in(arg_keys[7], 71), 0),
        "hand_rank": place_ends(jax.random.randint(arg_keys[6], (BOARDS, H), 0, 2000), jax.random.fold_in(arg_keys[6], 1), 0, 1999).astype(jnp.int32),
    }


DELTA = 0.05
EPSILON = 1e-06
DECK_SIZE = 52

def holding_table(hand_cards):
    deck_cards = jnp.arange(DECK_SIZE, dtype=jnp.int32)
    holding = (hand_cards[:, 0:1] == deck_cards[None, :]) | (hand_cards[:, 1:2] == deck_cards[None, :])
    return holding.astype(jnp.float32)

def board_free(board_cards, holding):
    deck_cards = jnp.arange(DECK_SIZE, dtype=jnp.int32)
    on_board = jnp.any(board_cards[:, :, None] == deck_cards[None, None, :], axis=1).astype(jnp.float32)
    touched = jnp.dot(on_board, holding.T, precision=lax.Precision.HIGHEST)
    return (touched < 0.5).astype(jnp.float32)

def payoff_matrix(rank_row, free_row, apart_mask):
    ranked = rank_row.astype(jnp.float32)
    sign_table = jnp.sign(ranked[:, None] - ranked[None, :])
    return sign_table * apart_mask * free_row[:, None] * free_row[None, :]

def node_totals(values, parents):
    totals = jax.ops.segment_sum(values, parents, num_segments=NODES)
    return totals[parents]

def reference(chance_reach, regrets_start, pot, parent, hand_cards, board_cards, hand_rank):
    holding = holding_table(hand_cards)
    apart_mask = (jnp.dot(holding, holding.T, precision=lax.Precision.HIGHEST) < 0.5).astype(jnp.float32)
    free_rows = board_free(board_cards, holding)
    pot_rows = pot.reshape(BOARDS, BOARD_LEAVES)
    regrets = regrets_start
    values = jnp.zeros_like(regrets_start)
    for iteration in range(ITERS):
        policy = []
        for player in range(2):
            positive = jnp.maximum(regrets[player], 0.0) + DELTA
            policy.append(positive / node_totals(positive, parent[player]))
        policy = jnp.stack(policy)
        own_reach = chance_reach * policy
        opposed = jnp.stack([own_reach[1], own_reach[0]]).reshape(2, BOARDS, BOARD_LEAVES, H).transpose(1, 0, 2, 3)

        def one_board(board_items):
            rank_row, free_row, opp_block, pot_row = board_items
            matrix = payoff_matrix(rank_row, free_row, apart_mask)
            summed = jnp.einsum('pkg,hg->pkh', opp_block, matrix, precision=lax.Precision.HIGHEST)
            return summed * (pot_row[None, :, None] * (1.0 / H))
        values = lax.map(one_board, (hand_rank, free_rows, opposed, pot_rows))
        values = values.transpose(1, 0, 2, 3).reshape(2, LEAVES, H)
        updated = []
        for player in range(2):
            instant = values[player] - node_totals(policy[player] * values[player], parent[player])
            norm_scale = jnp.sqrt(jnp.sum(instant * instant) / (LEAVES * H) + EPSILON)
            updated.append(regrets[player] + instant / norm_scale)
        regrets = jnp.stack(updated)
    return (regrets, values)
```

```python
import functools

import jax
import jax.numpy as jnp
from jax import lax
from jax.experimental import pallas as pl
from jax.experimental.pallas import tpu as pltpu
from jax.sharding import PartitionSpec as P

ITERS = 2
MOST = 6
DELTA = 0.05
EPSILON = 1e-06
DECK_SIZE = 52
LANES = 128
WIDE = 256
SPLIT = 4
PARTS = 2
MESH = pl.DeviceIdType.MESH
F32 = jnp.float32
BF16 = jnp.bfloat16

(GET_HALF, GET_BEFORE, GET_AFTER, GET_BEYOND, GET_CHANCE, GET_CHANCE_AFTER, GET_PARENT, GET_INFO,
 GET_LOW, GET_HIGH, GET_HIGHER, GET_VALUES, GET_EDGE_LOW, GET_EDGE_HIGH, GET_POLICY, GET_REGRETS, GETS) = (
    0, 1, 3, 5, 7, 8, 10, 11, 12, 13, 14, 15, 16, 17, 18, 19, 20)
(PUT_HALF, PUT_AFTER, PUT_BEFORE, PUT_BEYOND, PUT_CHANCE, PUT_CHANCE_BEFORE, PUT_PARENT, PUT_INFO,
 PUT_HIGH, PUT_LOW, PUT_LOWER, PUT_VALUES, PUT_EDGE, PUT_POLICY, PUT_REGRETS, PUTS) = (
    0, 1, 2, 3, 4, 5, 6, 7, 8, 9, 10, 11, 12, 14, 15, 16)


def round_up(value, unit):
    return (value + unit - 1) // unit * unit


def row_of(column, count):
    down = lax.broadcasted_iota(jnp.int32, (count, count), 0)
    across = lax.broadcasted_iota(jnp.int32, (count, count), 1)
    return jnp.sum(jnp.where(down == across, column, 0.0), axis=0, keepdims=True)


def same_of(ids):
    twice = jnp.concatenate([ids, ids], axis=0)
    return (ids == row_of(twice, twice.shape[0])).astype(BF16)


def node_totals(same, array):
    coarse = array.astype(BF16)
    fine = (array - coarse.astype(F32)).astype(BF16)
    return jnp.dot(same, jnp.concatenate([coarse, fine], axis=0), preferred_element_type=F32)


def settle(view, semaphore):
    pltpu.make_async_copy(view, view, semaphore).wait()


def body(
    n, boards, rows, hands, leaf_count,
    chance_far, regrets_far, pot_far, parent_far, cards_far, board_cards_far, rank_far,
    out_regrets, out_values,
    chance, regrets, pot, parents, cards, board_cards, rank, load,
    left, free, cards_wide, rank_wide, info, info_in, pots, weight,
    held, chances, policy, values, landed, standing_one, square_out, square_in,
    last_policy, last_regrets, last_values,
    all_in, put, get, square_send, square_recv,
    payoff, apart, turned, lows, right, same, same_own, same_last, split,
):
    me = lax.axis_index("leaf")
    player = lax.axis_index("player")
    other = 1 - player
    spot = 2 * me + player
    hub = 2 * n - 1
    width = free.shape[1]
    depth = left.shape[0]
    half = boards // 2
    near = half + 1
    local = boards * rows
    own = half * rows
    span = near * rows
    total = own + 3 * rows
    edge = min(MOST - 1, rows)
    rest = 2 * edge - rows
    last = ITERS - 1
    partner = {"player": other}

    def push(source, target, device, sent, received):
        pltpu.make_async_remote_copy(
            src_ref=source, dst_ref=target, send_sem=put.at[sent], recv_sem=get.at[received],
            device_id=device, device_id_type=MESH).start()

    def device_at(at):
        return {"leaf": at // 2, "player": at % 2}

    loads = [
        pltpu.make_async_copy(far, near_ref, load.at[i])
        for i, (far, near_ref) in enumerate((
            (cards_far, cards), (board_cards_far, board_cards), (rank_far, rank), (pot_far, pot), (regrets_far, regrets),
            (parent_far, parents.at[player]), (chance_far, chance)))]
    for copy in loads:
        copy.start()

    for p in range(2):
        held[p, :rows] = jnp.zeros((rows, hands), F32)
        held[p, rows + own :] = jnp.zeros((2 * rows, hands), F32)
        chances[p, own:] = jnp.zeros((rows, hands), F32)
        values[0, p, :rows] = jnp.zeros((rows, hands), F32)
        landed[p] = jnp.zeros((2 * rows, hands), F32)
    last_values[:rows] = jnp.zeros((rows, hands), F32)
    last_values[rows + local :] = jnp.zeros((rows, hands), F32)

    barrier = pltpu.get_barrier_semaphore()

    def greet(device):
        pl.semaphore_signal(barrier, inc=1, device_id=device, device_id_type=MESH)

    greet(partner)

    @pl.when((player == 0) & (me > 0))
    def _():
        for p in range(2):
            greet({"leaf": me - 1, "player": p})

    @pl.when((player == 1) & (me < n - 1))
    def _():
        for p in range(2):
            greet({"leaf": me + 1, "player": p})

    @pl.when(spot < hub - 2)
    def _():
        greet({"leaf": n - 1, "player": 1})

    for copy in loads[:4]:
        copy.wait()

    cards_wide[...] = jnp.full(cards_wide.shape, -1, jnp.int32)
    cards_wide[:, :hands] = cards[...]
    rank_wide[...] = jnp.zeros(rank_wide.shape, jnp.int32)
    rank_wide[:boards, :hands] = rank[...]
    card = lax.broadcasted_iota(jnp.int32, (depth, width), 0)
    lane = lax.broadcasted_iota(jnp.int32, (depth, width), 1)
    holding = ((card == cards_wide[0:1, :]) | (card == cards_wide[1:2, :])).astype(F32)
    valid = ((card == depth - 1) & (lane < hands)).astype(F32)
    ranked = rank_wide[...]
    code = ((128 + (ranked & 127)) << (ranked >> 7)).astype(F32)
    deck = lax.broadcasted_iota(jnp.int32, (boards, depth), 1)
    on_board = jnp.zeros((boards, depth), jnp.bool_)
    for k in range(board_cards.shape[1]):
        on_board = on_board | (deck == board_cards[:, k : k + 1])
    touched = jnp.dot(on_board.astype(BF16), holding.astype(BF16), preferred_element_type=F32)
    untouched = (touched < 0.5).astype(F32)
    first = player == 0
    left[...] = holding + valid
    left[DECK_SIZE : DECK_SIZE + half, :] = jnp.where(first, code[:half], code[half:boards])
    left[DECK_SIZE + half : DECK_SIZE + near, :] = code[half : half + 1]
    free[:half] = jnp.where(first, untouched[:half], untouched[half:])
    free[half:near] = untouched[half : half + 1]
    right[:, :width] = (valid - holding).astype(BF16)
    pick = lax.broadcasted_iota(jnp.int32, (depth, near * LANES), 0) - DECK_SIZE
    at_lane = lax.broadcasted_iota(jnp.int32, (depth, near * LANES), 1)
    right[:, width:] = ((at_lane >= pick * LANES) & (at_lane < pick * LANES + LANES)).astype(BF16)
    info[...] = jnp.zeros(info.shape, F32)
    info[:, :width] = code[:1]
    info[:, width : 2 * width] = untouched[:1]
    info[:, 2 * width : 2 * width + local] = pot[...]
    down = lax.broadcasted_iota(jnp.int32, (span, local), 0)
    across = lax.broadcasted_iota(jnp.int32, (span, local), 1)
    pots[...] = jnp.broadcast_to(
        jnp.sum(jnp.where(across == down + player * own, pot[...] * (1.0 / hands), 0.0), axis=1, keepdims=True),
        (span, LANES))
    split[...] = jnp.zeros(split.shape, BF16)

    turned[...] = left[...].T.astype(BF16)

    blocks = width // LANES
    length = width // PARTS

    def separate(first, last):
        for c in range(first, last, 2):
            found = jnp.dot(
                turned[...], right[:, c * LANES : min(c + 2, blocks) * LANES], preferred_element_type=F32).astype(BF16)
            for k in range(min(2, blocks - c)):
                apart[c + k] = found[:, k * LANES : (k + 1) * LANES].reshape(PARTS, length, LANES)

    def lower(begin, count):
        found = jnp.dot(
            turned[...], right[:, width + begin * LANES : width + (begin + count) * LANES],
            preferred_element_type=F32).astype(BF16)
        for b in range(count):
            lows[b] = found[:, b * LANES : (b + 1) * LANES].reshape(PARTS, length, LANES)

    def build(begin, count):
        def column(c, carry):
            at = pl.multiple_of(c * LANES, LANES)
            highs = [
                jnp.broadcast_to(
                    left[DECK_SIZE + begin + b : DECK_SIZE + begin + b + 1, pl.ds(at, LANES)], (16, LANES)).astype(BF16)
                for b in range(count)]

            def part(k, carry):
                for r in range(0, length, 16):
                    bound = apart[c, k, r : r + 16]
                    floor = -bound
                    for b in range(count):
                        gap = highs[b] - lows[b, k, r : r + 16]
                        payoff[begin + b, c, k, r : r + 16] = jnp.minimum(jnp.maximum(gap, floor), bound)
                return carry

            return lax.fori_loop(0, PARTS, part, carry)

        return column

    separate(0, blocks)
    lower(0, half)
    lax.fori_loop(0, SPLIT, build(0, half), 0)

    for copy in loads[4:]:
        copy.wait()

    @pl.when(spot < hub)
    def _():
        pl.semaphore_wait(barrier, 1 + (me > 0).astype(jnp.int32) + (me < n - 1).astype(jnp.int32))

    @pl.when(spot == hub)
    def _():
        pl.semaphore_wait(barrier, 2 * n - 1)

        def welcome(k, carry):
            pl.semaphore_signal(
                all_in, inc=1, device_id=device_at(lax.rem(spot + k, 2 * n)), device_id_type=MESH)
            return carry

        lax.fori_loop(1, 2 * n, welcome, 0)

    @pl.when(me > 0)
    def _():
        to = {"leaf": me - 1, "player": 1}

        @pl.when(player == 1)
        def _():
            push(info, info_in, to, PUT_INFO, GET_INFO)

        push(regrets.at[0, pl.ds(0, rows)], held.at[player, pl.ds(rows + own, rows)], to, PUT_BEFORE, GET_AFTER + player)
        push(
            regrets.at[0, pl.ds(rows, rest)], held.at[player, pl.ds(2 * rows + own, rest)], to, PUT_BEYOND,
            GET_BEYOND + player)
        push(chance.at[0, pl.ds(0, edge)], chances.at[player, pl.ds(own, edge)], to, PUT_CHANCE_BEFORE, GET_CHANCE_AFTER + player)

    @pl.when(me < n - 1)
    def _():
        push(
            regrets.at[0, pl.ds(local - edge, edge)], held.at[player, pl.ds(rows - edge, edge)],
            {"leaf": me + 1, "player": 0}, PUT_AFTER, GET_BEFORE + player)

    push(parents.at[player], parents.at[player], partner, PUT_PARENT, GET_PARENT)

    @pl.when(player == 0)
    def _():
        push(regrets.at[0, pl.ds(own - rows, own + rows)], held.at[0, pl.ds(0, own + rows)], partner, PUT_HALF, GET_HALF)
        push(chance.at[0, pl.ds(own, own)], chances.at[0, pl.ds(0, own)], partner, PUT_CHANCE, GET_CHANCE)
        held[0, rows:] = regrets[0, : own + 2 * rows]
        chances[0] = chance[0, :span]

    @pl.when(player == 1)
    def _():
        push(regrets.at[0, pl.ds(0, own + 2 * rows)], held.at[1, pl.ds(rows, own + 2 * rows)], partner, PUT_HALF, GET_HALF)
        push(chance.at[0, pl.ds(0, span)], chances.at[1], partner, PUT_CHANCE, GET_CHANCE)
        held[1, : own + rows] = regrets[0, own - rows :]
        chances[1, :own] = chance[0, own:]

    lax.fori_loop(SPLIT, blocks, build(0, half), 0)

    settle(parents.at[other], get.at[GET_PARENT])

    def ids_of(p, begin, count):
        leaf = begin + lax.broadcasted_iota(jnp.int32, (count, leaf_count), 0)
        here = lax.broadcasted_iota(jnp.int32, (count, leaf_count), 1)
        return jnp.sum(jnp.where(leaf == here, parents[p].astype(F32) + 1.0, 0.0), axis=1, keepdims=True)

    ids = []
    weights = []
    order = lax.broadcasted_iota(jnp.int32, (span, 1), 0)
    for p in range(2):
        found = ids_of(p, spot * own - rows, total)
        found = jnp.where(found > 0.0, found + p * (leaf_count + 1.0), 0.0)
        inside = found[rows : rows + span]
        counted = (inside > 0.0) & (inside != found[rows - 1 : rows])
        counted = counted & ((order < own) | (inside == found[rows + own - 1 : rows + own]))
        ids.append(found)
        weights.append(counted.astype(F32))
    same[...] = same_of(jnp.concatenate(ids, axis=0))
    same_own[...] = same_of(jnp.concatenate([found[rows : rows + span] for found in ids], axis=0))
    same_last[...] = same_of(ids_of(player, me * local - rows, local + 2 * rows))
    weight[...] = jnp.broadcast_to(jnp.concatenate(weights, axis=0), (2 * span, LANES))

    @pl.when((player == 1) & (me < n - 1))
    def _():
        settle(info_in, get.at[GET_INFO])
        left[DECK_SIZE + half : DECK_SIZE + near, :] = info_in[:, :width]
        free[half:near] = info_in[:, width : 2 * width]
        pots[own:] = jnp.broadcast_to(
            jnp.sum(
                jnp.where(across[:rows] == down[:rows], info_in[:, 2 * width : 2 * width + local] * (1.0 / hands), 0.0),
                axis=1, keepdims=True),
            (rows, LANES))

    turned[...] = left[...].T.astype(BF16)
    lower(half, 1)
    lax.fori_loop(0, blocks, build(half, 1), 0)

    @pl.when((player == 0) & (me > 0))
    def _():
        for p in range(2):
            settle(held.at[p, pl.ds(rows - edge, edge)], get.at[GET_BEFORE + p])

    @pl.when((player == 1) & (me < n - 1))
    def _():
        for p in range(2):
            settle(held.at[p, pl.ds(rows + own, rows)], get.at[GET_AFTER + p])
            settle(held.at[p, pl.ds(2 * rows + own, rest)], get.at[GET_BEYOND + p])
            settle(chances.at[p, pl.ds(own, edge)], get.at[GET_CHANCE_AFTER + p])

    @pl.when(player == 0)
    def _():
        settle(held.at[1, pl.ds(rows, own + 2 * rows)], get.at[GET_HALF])
        settle(chances.at[1], get.at[GET_CHANCE])

    @pl.when(player == 1)
    def _():
        settle(held.at[0, pl.ds(0, own + rows)], get.at[GET_HALF])
        settle(chances.at[0, pl.ds(0, own)], get.at[GET_CHANCE])

    standing = held[...].reshape(2 * total, hands)
    for it in range(ITERS):
        positive = jnp.maximum(standing, 0.0) + DELTA
        policy[it] = (positive / node_totals(same[...], positive)).reshape(2, total, hands)
        if it == last:
            standing_one[...] = standing.reshape(2, total, hands)
            push(
                policy.at[it, other, pl.ds(pl.multiple_of(player * rows, rows), span)],
                last_policy.at[pl.ds(pl.multiple_of(player * span, rows), span)], partner, PUT_POLICY, GET_POLICY)
            push(
                standing_one.at[other, pl.ds(rows, own)], last_regrets.at[pl.ds(pl.multiple_of(player * own, rows), own)],
                partner, PUT_REGRETS, GET_REGRETS)

        for b in range(near):
            seen = slice(b * rows, (b + 1) * rows)
            kept = slice((b + 1) * rows, (b + 2) * rows)
            open_hands = free[b : b + 1, :]
            facing = jnp.concatenate([chances[p, seen] * policy[it, p, kept] for p in range(2)], axis=0)
            facing = facing * open_hands[:, :hands]
            coarse = facing.astype(BF16).astype(F32)
            split[b, :, :hands] = jnp.concatenate([coarse, facing - coarse], axis=0).astype(BF16)
            summed = jnp.concatenate([
                jnp.dot(
                    split[b],
                    jnp.concatenate([payoff[b, k].reshape(width, LANES) for k in range(c, min(c + 2, blocks))], axis=1),
                    preferred_element_type=F32)
                for c in range(0, blocks, 2)], axis=1)
            stake = jnp.concatenate([pots[seen, :1]] * 2, axis=0)
            summed = (summed[: 2 * rows] + summed[2 * rows :])[:, :hands] + facing
            summed = summed * open_hands[:, :hands] * stake
            values[it, 1, kept] = summed[:rows]
            values[it, 0, kept] = summed[rows:]
            if b == half - 1 and it < last:
                @pl.when(spot < hub)
                def _(it=it):
                    push(
                        values.at[it, :, pl.ds(rows + own - edge, edge)], values.at[it, :, pl.ds(rows - edge, edge)],
                        device_at(spot + 1), PUT_HIGH, GET_LOW)

                @pl.when(spot > 0)
                def _(it=it):
                    push(
                        values.at[it, :, pl.ds(rows + edge, rows - edge)], landed.at[:, pl.ds(edge, rows - edge)],
                        device_at(spot - 1), PUT_LOW, GET_HIGH)
                    push(
                        values.at[it, :, pl.ds(2 * rows, rest)], landed.at[:, pl.ds(rows, rest)],
                        device_at(spot - 1), PUT_LOWER, GET_HIGHER)
            if b == half - 1 and it == last:
                push(
                    values.at[it, other, pl.ds(rows, own)],
                    last_values.at[pl.ds(pl.multiple_of(rows + player * own, rows), own)], partner, PUT_VALUES, GET_VALUES)

                @pl.when((player == 1) & (me < n - 1))
                def _(it=it):
                    for p in range(2):
                        push(
                            values.at[it, p, pl.ds(rows + own - edge, edge)], last_values.at[pl.ds(rows - edge, edge)],
                            {"leaf": me + 1, "player": p}, PUT_EDGE + p, GET_EDGE_LOW)

                @pl.when((player == 0) & (me > 0))
                def _(it=it):
                    for p in range(2):
                        push(
                            values.at[it, p, pl.ds(rows, edge)], last_values.at[pl.ds(rows + local, edge)],
                            {"leaf": me - 1, "player": p}, PUT_EDGE + p, GET_EDGE_HIGH)

        gained = jnp.concatenate([values[it, p, rows : rows + span] for p in range(2)], axis=0)
        played = jnp.concatenate([policy[it, p, rows : rows + span] for p in range(2)], axis=0)
        instant = (gained - node_totals(same_own[...], played * gained)) * weight[:, :1]
        squares = jnp.sum((instant * instant).reshape(2, span, hands), axis=1)
        square_out[it] = jnp.broadcast_to(jnp.sum(squares, axis=1, keepdims=True), (2, LANES))

        if it == 0:
            @pl.when(spot < hub)
            def _():
                pl.semaphore_wait(all_in, 1)

        def tell(k, carry, it=it):
            pltpu.make_async_remote_copy(
                src_ref=square_out.at[it], dst_ref=square_in.at[it, k - 1],
                send_sem=square_send.at[it], recv_sem=square_recv.at[it],
                device_id=device_at(lax.rem(spot + k, 2 * n)), device_id_type=MESH).start()
            return carry

        lax.fori_loop(1, 2 * n, tell, 0)

        if it < last:
            @pl.when(spot > 0)
            def _(it=it):
                settle(values.at[it, :, pl.ds(rows - edge, edge)], get.at[GET_LOW])

            @pl.when(spot < hub)
            def _():
                settle(landed.at[:, pl.ds(edge, rows - edge)], get.at[GET_HIGH])
                settle(landed.at[:, pl.ds(rows, rest)], get.at[GET_HIGHER])

            inner = lax.broadcasted_iota(jnp.int32, (rows, hands), 0) < edge
            gained = jnp.concatenate([
                part for p in range(2) for part in (
                    values[it, p, : rows + own], jnp.where(inner, values[it, p, rows + own : rows + span], landed[p, :rows]),
                    landed[p, rows:])], axis=0)
            instant = gained - node_totals(same[...], policy[it].reshape(2 * total, hands) * gained)
        else:
            mine = pl.ds(pl.multiple_of(player * span, rows), span)
            last_policy[mine] = policy[it, player, pl.ds(pl.multiple_of(player * rows, rows), span)]
            last_regrets[pl.ds(pl.multiple_of(player * own, rows), own)] = standing_one[player, pl.ds(rows, own)]
            last_values[pl.ds(pl.multiple_of(rows + player * own, rows), own)] = values[it, player, pl.ds(rows, own)]
            settle(last_policy.at[pl.ds(pl.multiple_of(other * span, rows), span)], get.at[GET_POLICY])
            settle(last_regrets.at[pl.ds(pl.multiple_of(other * own, rows), own)], get.at[GET_REGRETS])
            settle(last_values.at[pl.ds(pl.multiple_of(rows + other * own, rows), own)], get.at[GET_VALUES])

            @pl.when(me > 0)
            def _():
                settle(last_values.at[pl.ds(rows - edge, edge)], get.at[GET_EDGE_LOW])

            @pl.when(me < n - 1)
            def _():
                settle(last_values.at[pl.ds(rows + local, edge)], get.at[GET_EDGE_HIGH])

            gained = last_values[...]
            instant = (gained - node_totals(same_last[...], last_policy[...] * gained))[rows : rows + local]
            out_values[0] = gained[rows : rows + local]

        everyone = square_in.at[it]
        settle(everyone, square_recv.at[it])

        squares = square_out[it] + jnp.sum(square_in[it], axis=0)
        inverse = 1.0 / jnp.sqrt(squares / (leaf_count * hands) + EPSILON)
        if it < last:
            turn = lax.broadcasted_iota(jnp.int32, (2 * total, 1), 0) < total
            standing = standing + instant * jnp.where(turn, inverse[0:1, :1], inverse[1:2, :1])
        else:
            out_regrets[0] = last_regrets[...] + instant * jnp.where(player == 0, inverse[0:1, :1], inverse[1:2, :1])

    def sent(view, slot):
        settle(view, put.at[slot])

    @pl.when(me > 0)
    def _():
        @pl.when(player == 1)
        def _():
            sent(info, PUT_INFO)

        sent(regrets.at[0, pl.ds(0, rows)], PUT_BEFORE)
        sent(regrets.at[0, pl.ds(rows, rest)], PUT_BEYOND)
        sent(chance.at[0, pl.ds(0, edge)], PUT_CHANCE_BEFORE)

    @pl.when(me < n - 1)
    def _():
        sent(regrets.at[0, pl.ds(local - edge, edge)], PUT_AFTER)

    sent(parents.at[player], PUT_PARENT)

    @pl.when(player == 0)
    def _():
        sent(regrets.at[0, pl.ds(own - rows, own + rows)], PUT_HALF)
        sent(chance.at[0, pl.ds(own, own)], PUT_CHANCE)

    @pl.when(player == 1)
    def _():
        sent(regrets.at[0, pl.ds(0, own + 2 * rows)], PUT_HALF)
        sent(chance.at[0, pl.ds(0, span)], PUT_CHANCE)

    for it in range(last):
        @pl.when(spot < hub)
        def _(it=it):
            sent(values.at[it, :, pl.ds(rows + own - edge, edge)], PUT_HIGH)

        @pl.when(spot > 0)
        def _(it=it):
            sent(values.at[it, :, pl.ds(rows + edge, rows - edge)], PUT_LOW)
            sent(values.at[it, :, pl.ds(2 * rows, rest)], PUT_LOWER)

    sent(policy.at[last, other, pl.ds(pl.multiple_of(player * rows, rows), span)], PUT_POLICY)
    sent(standing_one.at[other, pl.ds(rows, own)], PUT_REGRETS)
    sent(values.at[last, other, pl.ds(rows, own)], PUT_VALUES)

    @pl.when((player == 1) & (me < n - 1))
    def _():
        for p in range(2):
            sent(values.at[last, p, pl.ds(rows + own - edge, edge)], PUT_EDGE + p)

    @pl.when((player == 0) & (me > 0))
    def _():
        for p in range(2):
            sent(values.at[last, p, pl.ds(rows, edge)], PUT_EDGE + p)

    for it in range(ITERS):
        everyone = square_in.at[it]
        settle(everyone, square_send.at[it])


def kernel(n, boards, rows, hands, leaf_count, *refs):
    near = boards // 2 + 1
    span = near * rows
    total = span + 2 * rows
    edged = (boards + 2) * rows
    width = round_up(hands, LANES)
    depth = round_up(DECK_SIZE + near + 1, 16)
    pl.run_scoped(
        functools.partial(body, n, boards, rows, hands, leaf_count, *refs),
        pltpu.VMEM((near, width // LANES, PARTS, width // PARTS, LANES), BF16),
        pltpu.VMEM((width // LANES, PARTS, width // PARTS, LANES), BF16),
        pltpu.VMEM((width, depth), BF16),
        pltpu.VMEM((near, PARTS, width // PARTS, LANES), BF16),
        pltpu.VMEM((depth, width + near * LANES), BF16),
        pltpu.VMEM((2 * total, 4 * total), BF16),
        pltpu.VMEM((2 * span, 4 * span), BF16),
        pltpu.VMEM((edged, 2 * edged), BF16),
        pltpu.VMEM((near, 4 * rows, width), BF16),
    )


def solution(mesh):
    n = mesh.shape["leaf"]

    def local(chance_reach, regrets_start, pot, parent, hand_cards, board_cards, hand_rank):
        leaf_rows, hands = chance_reach.shape[1:]
        boards = hand_rank.shape[0]
        rows = leaf_rows // boards
        leaf_count = parent.shape[1]
        width = round_up(hands, LANES)
        half = boards // 2
        near = half + 1
        depth = round_up(DECK_SIZE + near + 1, 16)
        span = near * rows
        total = (half + 3) * rows
        edged = leaf_rows + 2 * rows
        vmem = pl.BlockSpec(memory_space=pltpu.VMEM)
        shape = pltpu.VMEM(chance_reach.shape, F32)
        dma = pltpu.SemaphoreType.DMA
        arrays = (chance_reach, regrets_start, pot[None], parent, hand_cards.T, board_cards, hand_rank)
        return pl.pallas_call(
            functools.partial(kernel, n, boards, rows, hands, leaf_count),
            out_shape=(shape, shape),
            in_specs=[pl.BlockSpec(memory_space=pl.ANY)] * len(arrays),
            out_specs=(vmem, vmem),
            scratch_shapes=[
                pltpu.VMEM(chance_reach.shape, F32),
                pltpu.VMEM(regrets_start.shape, F32),
                pltpu.VMEM((1, leaf_rows), F32),
                pltpu.VMEM((2, 1, leaf_count), jnp.int32),
                pltpu.VMEM((2, hands), jnp.int32),
                pltpu.VMEM(board_cards.shape, jnp.int32),
                pltpu.VMEM(hand_rank.shape, jnp.int32),
                dma((len(arrays),)),
                pltpu.VMEM((depth, width), F32),
                pltpu.VMEM((near, width), F32),
                pltpu.VMEM((2, width), jnp.int32),
                pltpu.VMEM((round_up(boards, 8), width), jnp.int32),
                pltpu.VMEM((1, 2 * width + LANES), F32),
                pltpu.VMEM((1, 2 * width + LANES), F32),
                pltpu.VMEM((span, LANES), F32),
                pltpu.VMEM((2 * span, LANES), F32),
                pltpu.VMEM((2, total, hands), F32),
                pltpu.VMEM((2, span, hands), F32),
                pltpu.VMEM((ITERS, 2, total, hands), F32),
                pltpu.VMEM((ITERS, 2, total, hands), F32),
                pltpu.VMEM((2, 2 * rows, hands), F32),
                pltpu.VMEM((2, total, hands), F32),
                pltpu.VMEM((ITERS, 2, LANES), F32),
                pltpu.VMEM((ITERS, 2 * n - 1, 2, LANES), F32),
                pltpu.VMEM((edged, hands), F32),
                pltpu.VMEM((leaf_rows, hands), F32),
                pltpu.VMEM((edged, hands), F32),
                pltpu.SemaphoreType.REGULAR,
                dma((PUTS,)), dma((GETS,)),
                dma((ITERS,)), dma((ITERS,)),
            ],
            compiler_params=pltpu.CompilerParams(collective_id=0, has_side_effects=True),
            name="regret",
        )(*arrays)

    in_specs = (
        P("player", "leaf", None),
        P("player", "leaf", None),
        P("leaf"),
        P("player", None),
        P(),
        P("leaf", None),
        P("leaf", None),
    )
    out_specs = (P("player", "leaf", None), P("player", "leaf", None))
    return jax.shard_map(local, mesh=mesh, in_specs=in_specs, out_specs=out_specs, check_vma=False)
```

```python
import functools

import jax
import jax.numpy as jnp
from jax import lax
from jax.experimental import pallas as pl
from jax.experimental.pallas import tpu as pltpu
from jax.sharding import PartitionSpec as P

ITERS = 2
MOST = 6
DELTA = 0.05
EPSILON = 1e-06
DECK_SIZE = 52
LANES = 128
WIDE = 256
PARTS = 2
MESH = pl.DeviceIdType.MESH
F32 = jnp.float32
BF16 = jnp.bfloat16
F8 = jnp.float8_e4m3fn

(GET_HALF, GET_BEHIND, GET_NEXT, GET_AHEAD, GET_LATE, GET_AFTER, GET_BEYOND, GET_CHANCE, GET_CHANCE_AFTER, GET_PARENT,
 GET_INFO, GET_LOW, GET_HIGH, GET_HIGHER, GET_VALUES, GET_EDGE_LOW, GET_EDGE_HIGH, GET_POLICY, GET_REGRETS, GETS) = (
    0, 1, 3, 5, 7, 9, 11, 13, 14, 16, 17, 18, 19, 20, 21, 22, 23, 24, 25, 26)
(PUT_HALF, PUT_BEHIND, PUT_NEXT, PUT_AHEAD, PUT_LATE, PUT_AFTER, PUT_BEYOND, PUT_CHANCE, PUT_CHANCE_BEFORE, PUT_PARENT,
 PUT_INFO, PUT_HIGH, PUT_LOW, PUT_LOWER, PUT_VALUES, PUT_EDGE, PUT_POLICY, PUT_REGRETS, PUTS) = (
    0, 1, 2, 3, 4, 5, 6, 7, 8, 9, 10, 11, 12, 13, 14, 15, 17, 18, 19)


def round_up(value, unit):
    return (value + unit - 1) // unit * unit


def row_of(column, count):
    down = lax.broadcasted_iota(jnp.int32, (count, count), 0)
    across = lax.broadcasted_iota(jnp.int32, (count, count), 1)
    return jnp.sum(jnp.where(down == across, column, 0.0), axis=0, keepdims=True)


def same_of(ids):
    twice = jnp.concatenate([ids, ids], axis=0)
    return (ids == row_of(twice, twice.shape[0])).astype(BF16)


def node_totals(same, array):
    coarse = array.astype(BF16)
    fine = (array - coarse.astype(F32)).astype(BF16)
    return jnp.dot(same, jnp.concatenate([coarse, fine], axis=0), preferred_element_type=F32)


def settle(view, semaphore):
    pltpu.make_async_copy(view, view, semaphore).wait()


def body(
    n, boards, rows, hands, leaf_count,
    chance_far, regrets_far, pot_far, parent_far, cards_far, board_cards_far, rank_far,
    outs,
    chance, regrets, pot, parents, cards, board_cards, rank, load,
    codes, free, cards_wide, rank_wide, info, info_in, pots, weight,
    held, chances, policy, values, landed, standing_one, square_out, square_in,
    last_policy, last_regrets, last_values, reach, behind, behind_out, ahead, ahead_out, late_before, late_after,
    all_in, put, get, square_send, square_recv,
    payoff, apart, turned, lows, right, same, same_own, same_last, split,
):
    me = lax.axis_index("leaf")
    player = lax.axis_index("player")
    other = 1 - player
    spot = 2 * me + player
    hub = 2 * n - 1
    width = free.shape[1]
    depth = right.shape[0]
    half = boards // 2
    near = half + 1
    local = boards * rows
    own = half * rows
    span = near * rows
    total = own + 3 * rows
    edge = min(MOST - 1, rows)
    rest = 2 * edge - rows
    last = ITERS - 1
    partner = {"player": other}

    def push(source, target, device, sent, received):
        pltpu.make_async_remote_copy(
            src_ref=source, dst_ref=target, send_sem=put.at[sent], recv_sem=get.at[received],
            device_id=device, device_id_type=MESH).start()

    def device_at(at):
        return {"leaf": at // 2, "player": at % 2}

    loads = [
        pltpu.make_async_copy(far, near_ref, load.at[i])
        for i, (far, near_ref) in enumerate((
            (cards_far, cards), (board_cards_far, board_cards), (rank_far, rank), (pot_far, pot), (regrets_far, regrets),
            (parent_far, parents.at[player]), (chance_far, chance)))]
    for copy in loads:
        copy.start()

    for p in range(2):
        held[p, :rows] = jnp.zeros((rows, hands), F32)
        held[p, rows + own :] = jnp.zeros((2 * rows, hands), F32)
        chances[p, own:] = jnp.zeros((rows, hands), F32)
        values[0, p, :rows] = jnp.zeros((rows, hands), F32)
        landed[p] = jnp.zeros((2 * rows, hands), F32)
        behind[p] = jnp.zeros((1, hands), F32)
        ahead[p] = jnp.zeros((rows, hands), F32)
        late_before[p] = jnp.zeros((rows, hands), F32)
        late_after[p] = jnp.zeros((2 * rows, hands), F32)
    last_values[:rows] = jnp.zeros((rows, hands), F32)
    last_values[rows + local :] = jnp.zeros((rows, hands), F32)

    barrier = pltpu.get_barrier_semaphore()

    def greet(device):
        pl.semaphore_signal(barrier, inc=1, device_id=device, device_id_type=MESH)

    greet(partner)

    @pl.when((player == 0) & (me > 0))
    def _():
        for p in range(2):
            greet({"leaf": me - 1, "player": p})

    @pl.when((player == 1) & (me < n - 1))
    def _():
        for p in range(2):
            greet({"leaf": me + 1, "player": p})

    @pl.when(spot < hub - 2)
    def _():
        greet({"leaf": n - 1, "player": 1})

    for copy in loads[:4]:
        copy.wait()

    cards_wide[...] = jnp.full(cards_wide.shape, -1, jnp.int32)
    cards_wide[:, :hands] = cards[...]
    rank_wide[...] = jnp.zeros(rank_wide.shape, jnp.int32)
    rank_wide[:boards, :hands] = rank[...]
    card = lax.broadcasted_iota(jnp.int32, (depth, width), 0)
    lane = lax.broadcasted_iota(jnp.int32, (depth, width), 1)
    holding = ((card == cards_wide[0:1, :]) | (card == cards_wide[1:2, :])).astype(F32)
    valid = ((card == depth - 1) & (lane < hands)).astype(F32)
    ranked = rank_wide[...]
    code = ((128 + (ranked & 127)) << (ranked >> 7)).astype(F32)
    deck = lax.broadcasted_iota(jnp.int32, (boards, depth), 1)
    on_board = jnp.zeros((boards, depth), jnp.bool_)
    for k in range(board_cards.shape[1]):
        on_board = on_board | (deck == board_cards[:, k : k + 1])
    touched = jnp.dot(on_board.astype(BF16), holding.astype(BF16), preferred_element_type=F32)
    untouched = (touched < 0.5).astype(F32)
    first = player == 0
    turned[...] = (holding + valid).T.astype(F8)
    codes[...] = jnp.zeros(codes.shape, F32)
    codes[:half] = jnp.where(first, code[:half], code[half:boards])
    codes[half:near] = code[half : half + 1]
    free[:half] = jnp.where(first, untouched[:half], untouched[half:])
    free[half:near] = untouched[half : half + 1]
    right[...] = (valid - holding).astype(F8)
    info[...] = jnp.zeros(info.shape, F32)
    info[:, :width] = code[:1]
    info[:, width : 2 * width] = untouched[:1]
    info[:, 2 * width : 2 * width + local] = pot[...]
    down = lax.broadcasted_iota(jnp.int32, (span, local), 0)
    across = lax.broadcasted_iota(jnp.int32, (span, local), 1)
    pots[...] = jnp.broadcast_to(
        jnp.sum(jnp.where(across == down + player * own, pot[...] * (1.0 / hands), 0.0), axis=1, keepdims=True),
        (span, LANES))
    split[...] = jnp.zeros(split.shape, BF16)

    blocks = width // LANES
    length = width // PARTS

    def separate(first, last):
        for c in range(first, last, 2):
            found = jnp.dot(
                turned[...], right[:, c * LANES : min(c + 2, blocks) * LANES], preferred_element_type=F32).astype(BF16)
            for k in range(min(2, blocks - c)):
                apart[c + k] = found[:, k * LANES : (k + 1) * LANES].reshape(PARTS, length, LANES)

    def lower(begin, count):
        columns = codes[...].T
        for b in range(count):
            lows[b] = jnp.broadcast_to(
                columns[:, begin + b : begin + b + 1], (width, LANES)).astype(BF16).reshape(PARTS, length, LANES)

    def build(begin, count):
        def column(c, carry):
            at = pl.multiple_of(c * LANES, LANES)
            highs = [
                jnp.broadcast_to(
                    codes[begin + b : begin + b + 1, pl.ds(at, LANES)], (32, LANES)).astype(BF16)
                for b in range(count)]

            def part(k, carry):
                for r in range(0, length, 32):
                    bound = apart[c, k, r : r + 32]
                    floor = -bound
                    for b in range(count):
                        gap = highs[b] - lows[b, k, r : r + 32]
                        payoff[begin + b, c, k, r : r + 32] = jnp.minimum(jnp.maximum(gap, floor), bound).astype(F8)
                return carry

            return lax.fori_loop(0, PARTS, part, carry)

        return column

    for copy in loads[4:]:
        copy.wait()

    def ids_of(p, begin, count):
        leaf = begin + lax.broadcasted_iota(jnp.int32, (count, leaf_count), 0)
        here = lax.broadcasted_iota(jnp.int32, (count, leaf_count), 1)
        return jnp.sum(jnp.where(leaf == here, parents[p].astype(F32) + 1.0, 0.0), axis=1, keepdims=True)

    found = ids_of(player, me * local - rows, 3 * rows)
    positive = jnp.maximum(regrets[0, : 2 * rows], 0.0) + DELTA
    shared = (found[rows : 2 * rows] == found[rows - 1 : rows]) & (found[rows - 1 : rows] > 0.0)
    partial = node_totals(same_of(found[rows:]), positive)[:rows]
    ahead_out[...] = chance[0, :rows] * positive[:rows] / jnp.where(shared, 1.0, partial)
    found = ids_of(player, (me + 1) * local - rows, rows)
    positive = jnp.maximum(regrets[0, local - rows :], 0.0) + DELTA
    behind_out[...] = jnp.sum(jnp.where(found == found[rows - 1 :], positive, 0.0), axis=0, keepdims=True)

    @pl.when(me == 0)
    def _():
        separate(0, blocks)

    @pl.when(spot < hub)
    def _():
        pl.semaphore_wait(barrier, 1 + (me > 0).astype(jnp.int32) + (me < n - 1).astype(jnp.int32))

    @pl.when(spot == hub)
    def _():
        pl.semaphore_wait(barrier, 2 * n - 1)

    @pl.when(me < n - 1)
    def _():
        push(behind_out, behind.at[player], {"leaf": me + 1, "player": 0}, PUT_BEHIND, GET_BEHIND + player)

    @pl.when(me > 0)
    def _():
        to = {"leaf": me - 1, "player": 1}

        @pl.when(player == 1)
        def _():
            push(info, info_in, to, PUT_INFO, GET_INFO)

        push(regrets.at[0, pl.ds(0, edge)], held.at[player, pl.ds(rows + own, edge)], to, PUT_NEXT, GET_NEXT + player)
        push(ahead_out.at[pl.ds(0, edge)], ahead.at[player, pl.ds(0, edge)], to, PUT_AHEAD, GET_AHEAD + player)

    push(parents.at[player], parents.at[player], partner, PUT_PARENT, GET_PARENT)

    @pl.when(player == 0)
    def _():
        push(regrets.at[0, pl.ds(own - rows, own + rows)], held.at[0, pl.ds(0, own + rows)], partner, PUT_HALF, GET_HALF)
        push(chance.at[0, pl.ds(own, own)], chances.at[0, pl.ds(0, own)], partner, PUT_CHANCE, GET_CHANCE)
        held[0, rows:] = regrets[0, : own + 2 * rows]
        chances[0] = chance[0, :span]

    @pl.when(player == 1)
    def _():
        push(regrets.at[0, pl.ds(0, own + 2 * rows)], held.at[1, pl.ds(rows, own + 2 * rows)], partner, PUT_HALF, GET_HALF)
        push(chance.at[0, pl.ds(0, span)], chances.at[1], partner, PUT_CHANCE, GET_CHANCE)
        held[1, : own + rows] = regrets[0, own - rows :]
        chances[1, :own] = chance[0, own:]

    @pl.when(spot == hub)
    def _():
        def welcome(k, carry):
            pl.semaphore_signal(
                all_in, inc=1, device_id=k - 1, device_id_type=pl.DeviceIdType.LOGICAL)
            return carry

        lax.fori_loop(1, 2 * n, welcome, 0)

    @pl.when(me > 0)
    def _():
        separate(0, blocks)

    lower(0, half)
    lax.fori_loop(0, blocks, build(0, half), 0)

    @pl.when(me < n - 1)
    def _():
        push(
            regrets.at[0, pl.ds(local - edge, edge)], late_before.at[player, pl.ds(rows - edge, edge)],
            {"leaf": me + 1, "player": 0}, PUT_LATE, GET_LATE + player)

    @pl.when(me > 0)
    def _():
        to = {"leaf": me - 1, "player": 1}
        push(
            regrets.at[0, pl.ds(edge, rows - edge)], late_after.at[player, pl.ds(edge, rows - edge)], to, PUT_AFTER,
            GET_AFTER + player)
        push(
            regrets.at[0, pl.ds(rows, rest)], late_after.at[player, pl.ds(rows, rest)], to, PUT_BEYOND,
            GET_BEYOND + player)

    settle(parents.at[other], get.at[GET_PARENT])

    ids = []
    weights = []
    order = lax.broadcasted_iota(jnp.int32, (span, 1), 0)
    for p in range(2):
        found = ids_of(p, spot * own - rows, total)
        found = jnp.where(found > 0.0, found + p * (leaf_count + 1.0), 0.0)
        inside = found[rows : rows + span]
        counted = (inside > 0.0) & (inside != found[rows - 1 : rows])
        counted = counted & ((order < own) | (inside == found[rows + own - 1 : rows + own]))
        ids.append(found)
        weights.append(counted.astype(F32))
    same[...] = same_of(jnp.concatenate(ids, axis=0))
    same_own[...] = same_of(jnp.concatenate([found[rows : rows + span] for found in ids], axis=0))
    same_last[...] = same_of(ids_of(player, me * local - rows, local + 2 * rows))
    weight[...] = jnp.broadcast_to(jnp.concatenate(weights, axis=0), (2 * span, LANES))

    @pl.when((player == 1) & (me < n - 1))
    def _():
        settle(info_in, get.at[GET_INFO])
        codes[half:near] = info_in[:, :width]
        free[half:near] = info_in[:, width : 2 * width]
        pots[own:] = jnp.broadcast_to(
            jnp.sum(
                jnp.where(across[:rows] == down[:rows], info_in[:, 2 * width : 2 * width + local] * (1.0 / hands), 0.0),
                axis=1, keepdims=True),
            (rows, LANES))

    lower(half, 1)
    lax.fori_loop(0, blocks, build(half, 1), 0)

    @pl.when((player == 0) & (me > 0))
    def _():
        for p in range(2):
            settle(behind.at[p], get.at[GET_BEHIND + p])

    @pl.when((player == 1) & (me < n - 1))
    def _():
        for p in range(2):
            settle(held.at[p, pl.ds(rows + own, edge)], get.at[GET_NEXT + p])
            settle(ahead.at[p, pl.ds(0, edge)], get.at[GET_AHEAD + p])

    @pl.when(player == 0)
    def _():
        settle(held.at[1, pl.ds(rows, own + 2 * rows)], get.at[GET_HALF])
        settle(chances.at[1], get.at[GET_CHANCE])

    @pl.when(player == 1)
    def _():
        settle(held.at[0, pl.ds(0, own + rows)], get.at[GET_HALF])
        settle(chances.at[0, pl.ds(0, own)], get.at[GET_CHANCE])

    def strategy(standing):
        positive = jnp.maximum(standing, 0.0) + DELTA
        return positive / node_totals(same[...], positive)

    for it in range(ITERS):
        if it == 0:
            at = lax.broadcasted_iota(jnp.int32, (2 * total, 1), 0)
            at = jnp.where(at >= total, at - total, at)
            present = ((player == 0) & (at >= rows)) | ((player == 1) & (at < rows + own + edge))
            positive = jnp.where(present, jnp.maximum(held[...].reshape(2 * total, hands), 0.0) + DELTA, 0.0)
            totals = node_totals(same[...], positive)
            for p in range(2):
                found = ids[p]
                mine = slice(p * total + rows, p * total + rows + own)
                beside = slice(mine.stop, mine.stop + rows)
                back = (found[rows : rows + own] == found[rows - 1 : rows]) & (found[rows - 1 : rows] > 0.0)
                forth = found[rows + own : rows + span] == found[rows + own - 1 : rows + own]
                choice = positive[mine] / (totals[mine] + jnp.where(back, behind[p], 0.0))
                policy[0, p, rows : rows + own] = choice
                reach[p, :own] = chances[p, :own] * choice
                policy[0, p, rows + own : rows + span] = positive[beside] / jnp.where(forth, totals[beside], 1.0)
                reach[p, own:] = jnp.where(player == 0, chances[p, own:] * positive[beside], ahead[p]) / jnp.where(
                    forth | (player == 0), totals[beside], 1.0)
        else:
            policy[it] = strategy(standing).reshape(2, total, hands)
            for p in range(2):
                reach[p, :own] = chances[p, :own] * policy[it, p, rows : rows + own]
                reach[p, own:] = chances[p, own:] * policy[it, p, rows + own : rows + span]
        if it == last:
            standing_one[...] = standing.reshape(2, total, hands)
            push(
                policy.at[it, other, pl.ds(pl.multiple_of(player * rows, rows), span)],
                last_policy.at[pl.ds(pl.multiple_of(player * span, rows), span)], partner, PUT_POLICY, GET_POLICY)
            push(
                standing_one.at[other, pl.ds(rows, own)], last_regrets.at[pl.ds(pl.multiple_of(player * own, rows), own)],
                partner, PUT_REGRETS, GET_REGRETS)

        for b in range(near):
            seen = slice(b * rows, (b + 1) * rows)
            kept = slice((b + 1) * rows, (b + 2) * rows)
            open_hands = free[b : b + 1, :]
            facing = jnp.concatenate([reach[p, seen] for p in range(2)], axis=0)
            facing = facing * open_hands[:, :hands]
            coarse = facing.astype(BF16).astype(F32)
            split[b, :, :hands] = jnp.concatenate([coarse, facing - coarse], axis=0).astype(BF16)
            summed = jnp.concatenate([
                jnp.dot(
                    split[b],
                    jnp.concatenate([payoff[b, k].reshape(width, LANES) for k in range(c, min(c + 2, blocks))], axis=1),
                    preferred_element_type=F32)
                for c in range(0, blocks, 2)], axis=1)
            stake = jnp.concatenate([pots[seen, :1]] * 2, axis=0)
            summed = (summed[: 2 * rows] + summed[2 * rows :])[:, :hands] + facing
            summed = summed * open_hands[:, :hands] * stake
            values[it, 1, kept] = summed[:rows]
            values[it, 0, kept] = summed[rows:]
            if b == half - 1 and it < last:
                @pl.when(spot < hub)
                def _(it=it):
                    push(
                        values.at[it, :, pl.ds(rows + own - edge, edge)], values.at[it, :, pl.ds(rows - edge, edge)],
                        device_at(spot + 1), PUT_HIGH, GET_LOW)

                @pl.when(spot > 0)
                def _(it=it):
                    push(
                        values.at[it, :, pl.ds(rows + edge, rows - edge)], landed.at[:, pl.ds(edge, rows - edge)],
                        device_at(spot - 1), PUT_LOW, GET_HIGH)
                    push(
                        values.at[it, :, pl.ds(2 * rows, rest)], landed.at[:, pl.ds(rows, rest)],
                        device_at(spot - 1), PUT_LOWER, GET_HIGHER)
            if b == half - 1 and it == last:
                push(
                    values.at[it, other, pl.ds(rows, own)],
                    last_values.at[pl.ds(pl.multiple_of(rows + player * own, rows), own)], partner, PUT_VALUES, GET_VALUES)

                @pl.when((player == 1) & (me < n - 1))
                def _(it=it):
                    for p in range(2):
                        push(
                            values.at[it, p, pl.ds(rows + own - edge, edge)], last_values.at[pl.ds(rows - edge, edge)],
                            {"leaf": me + 1, "player": p}, PUT_EDGE + p, GET_EDGE_LOW)

                @pl.when((player == 0) & (me > 0))
                def _(it=it):
                    for p in range(2):
                        push(
                            values.at[it, p, pl.ds(rows, edge)], last_values.at[pl.ds(rows + local, edge)],
                            {"leaf": me - 1, "player": p}, PUT_EDGE + p, GET_EDGE_HIGH)

        gained = jnp.concatenate([values[it, p, rows : rows + span] for p in range(2)], axis=0)
        played = jnp.concatenate([policy[it, p, rows : rows + span] for p in range(2)], axis=0)
        instant = (gained - node_totals(same_own[...], played * gained)) * weight[:, :1]
        squares = jnp.sum((instant * instant).reshape(2, span, hands), axis=1)
        square_out[it] = jnp.broadcast_to(jnp.sum(squares, axis=1, keepdims=True), (2, LANES))

        if it == 0:
            @pl.when(spot < hub)
            def _():
                pl.semaphore_wait(all_in, 1)

        def tell(t, carry, it=it):
            at = t if it == last else jnp.where(spot < n, 2 * n - 2 - t, t)
            ahead = (at >= spot).astype(jnp.int32)
            pltpu.make_async_remote_copy(
                src_ref=square_out.at[it], dst_ref=square_in.at[it, spot - 1 + ahead],
                send_sem=square_send.at[it], recv_sem=square_recv.at[it],
                device_id=at + ahead, device_id_type=pl.DeviceIdType.LOGICAL).start()
            return carry

        lax.fori_loop(0, 2 * n - 1, tell, 0)

        if it == 0:
            @pl.when((player == 0) & (me > 0))
            def _():
                for p in range(2):
                    settle(late_before.at[p, pl.ds(rows - edge, edge)], get.at[GET_LATE + p])

            @pl.when((player == 1) & (me < n - 1))
            def _():
                for p in range(2):
                    settle(late_after.at[p, pl.ds(edge, rows - edge)], get.at[GET_AFTER + p])
                    settle(late_after.at[p, pl.ds(rows, rest)], get.at[GET_BEYOND + p])

            standing = jnp.concatenate([
                part for p in range(2) for part in (
                    held[p, :rows] + late_before[p], held[p, rows : rows + own],
                    held[p, rows + own :] + late_after[p])], axis=0)
            policy[0] = strategy(standing).reshape(2, total, hands)
            for p in range(2):
                beside = slice(p * total + rows + own, p * total + rows + span)
                forth = ids[p][rows + own : rows + span] == ids[p][rows + own - 1 : rows + own]
                factor = jnp.where(forth, jnp.maximum(standing[beside], 0.0) + DELTA, policy[0, p, rows + own : rows + span])
                chances[p, own:] = jnp.where(player == 0, chances[p, own:], ahead[p] / factor)

        if it < last:
            @pl.when(spot > 0)
            def _(it=it):
                settle(values.at[it, :, pl.ds(rows - edge, edge)], get.at[GET_LOW])

            @pl.when(spot < hub)
            def _():
                settle(landed.at[:, pl.ds(edge, rows - edge)], get.at[GET_HIGH])
                settle(landed.at[:, pl.ds(rows, rest)], get.at[GET_HIGHER])

            inner = lax.broadcasted_iota(jnp.int32, (rows, hands), 0) < edge
            gained = jnp.concatenate([
                part for p in range(2) for part in (
                    values[it, p, : rows + own], jnp.where(inner, values[it, p, rows + own : rows + span], landed[p, :rows]),
                    landed[p, rows:])], axis=0)
            instant = gained - node_totals(same[...], policy[it].reshape(2 * total, hands) * gained)
        else:
            mine = pl.ds(pl.multiple_of(player * span, rows), span)
            last_policy[mine] = policy[it, player, pl.ds(pl.multiple_of(player * rows, rows), span)]
            last_regrets[pl.ds(pl.multiple_of(player * own, rows), own)] = standing_one[player, pl.ds(rows, own)]
            last_values[pl.ds(pl.multiple_of(rows + player * own, rows), own)] = values[it, player, pl.ds(rows, own)]
            settle(last_policy.at[pl.ds(pl.multiple_of(other * span, rows), span)], get.at[GET_POLICY])
            settle(last_regrets.at[pl.ds(pl.multiple_of(other * own, rows), own)], get.at[GET_REGRETS])
            settle(last_values.at[pl.ds(pl.multiple_of(rows + other * own, rows), own)], get.at[GET_VALUES])

            @pl.when(me > 0)
            def _():
                settle(last_values.at[pl.ds(rows - edge, edge)], get.at[GET_EDGE_LOW])

            @pl.when(me < n - 1)
            def _():
                settle(last_values.at[pl.ds(rows + local, edge)], get.at[GET_EDGE_HIGH])

            gained = last_values[...]
            instant = (gained - node_totals(same_last[...], last_policy[...] * gained))[rows : rows + local]
            outs[1] = gained[rows : rows + local]

        everyone = square_in.at[it]
        settle(everyone, square_recv.at[it])

        squares = square_out[it] + jnp.sum(square_in[it], axis=0)
        inverse = 1.0 / jnp.sqrt(squares / (leaf_count * hands) + EPSILON)
        if it < last:
            turn = lax.broadcasted_iota(jnp.int32, (2 * total, 1), 0) < total
            standing = standing + instant * jnp.where(turn, inverse[0:1, :1], inverse[1:2, :1])
        else:
            outs[0] = last_regrets[...] + instant * jnp.where(player == 0, inverse[0:1, :1], inverse[1:2, :1])

    def sent(view, slot):
        settle(view, put.at[slot])

    @pl.when(me > 0)
    def _():
        @pl.when(player == 1)
        def _():
            sent(info, PUT_INFO)

        sent(regrets.at[0, pl.ds(0, edge)], PUT_NEXT)
        sent(ahead_out.at[pl.ds(0, edge)], PUT_AHEAD)
        sent(regrets.at[0, pl.ds(edge, rows - edge)], PUT_AFTER)
        sent(regrets.at[0, pl.ds(rows, rest)], PUT_BEYOND)

    @pl.when(me < n - 1)
    def _():
        sent(behind_out, PUT_BEHIND)
        sent(regrets.at[0, pl.ds(local - edge, edge)], PUT_LATE)

    sent(parents.at[player], PUT_PARENT)

    @pl.when(player == 0)
    def _():
        sent(regrets.at[0, pl.ds(own - rows, own + rows)], PUT_HALF)
        sent(chance.at[0, pl.ds(own, own)], PUT_CHANCE)

    @pl.when(player == 1)
    def _():
        sent(regrets.at[0, pl.ds(0, own + 2 * rows)], PUT_HALF)
        sent(chance.at[0, pl.ds(0, span)], PUT_CHANCE)

    for it in range(last):
        @pl.when(spot < hub)
        def _(it=it):
            sent(values.at[it, :, pl.ds(rows + own - edge, edge)], PUT_HIGH)

        @pl.when(spot > 0)
        def _(it=it):
            sent(values.at[it, :, pl.ds(rows + edge, rows - edge)], PUT_LOW)
            sent(values.at[it, :, pl.ds(2 * rows, rest)], PUT_LOWER)

    sent(policy.at[last, other, pl.ds(pl.multiple_of(player * rows, rows), span)], PUT_POLICY)
    sent(standing_one.at[other, pl.ds(rows, own)], PUT_REGRETS)
    sent(values.at[last, other, pl.ds(rows, own)], PUT_VALUES)

    @pl.when((player == 1) & (me < n - 1))
    def _():
        for p in range(2):
            sent(values.at[last, p, pl.ds(rows + own - edge, edge)], PUT_EDGE + p)

    @pl.when((player == 0) & (me > 0))
    def _():
        for p in range(2):
            sent(values.at[last, p, pl.ds(rows, edge)], PUT_EDGE + p)

    for it in range(ITERS):
        everyone = square_in.at[it]
        settle(everyone, square_send.at[it])


def kernel(n, boards, rows, hands, leaf_count, *refs):
    near = boards // 2 + 1
    span = near * rows
    total = span + 2 * rows
    edged = (boards + 2) * rows
    width = round_up(hands, LANES)
    depth = round_up(DECK_SIZE + 1, 32)
    pl.run_scoped(
        functools.partial(body, n, boards, rows, hands, leaf_count, *refs),
        pltpu.VMEM((near, width // LANES, PARTS, width // PARTS, LANES), F8),
        pltpu.VMEM((width // LANES, PARTS, width // PARTS, LANES), BF16),
        pltpu.VMEM((width, depth), F8),
        pltpu.VMEM((near, PARTS, width // PARTS, LANES), BF16),
        pltpu.VMEM((depth, width), F8),
        pltpu.VMEM((2 * total, 4 * total), BF16),
        pltpu.VMEM((2 * span, 4 * span), BF16),
        pltpu.VMEM((edged, 2 * edged), BF16),
        pltpu.VMEM((near, 4 * rows, width), BF16),
    )


def solution(mesh):
    n = mesh.shape["leaf"]

    def local(chance_reach, regrets_start, pot, parent, hand_cards, board_cards, hand_rank):
        leaf_rows, hands = chance_reach.shape[1:]
        boards = hand_rank.shape[0]
        rows = leaf_rows // boards
        leaf_count = parent.shape[1]
        width = round_up(hands, LANES)
        half = boards // 2
        near = half + 1
        span = near * rows
        total = (half + 3) * rows
        edged = leaf_rows + 2 * rows
        vmem = pl.BlockSpec(memory_space=pltpu.VMEM)
        shape = pltpu.VMEM(chance_reach.shape, F32)
        dma = pltpu.SemaphoreType.DMA
        arrays = (chance_reach, regrets_start, pot[None], parent, hand_cards.T, board_cards, hand_rank)
        outs = pl.pallas_call(
            functools.partial(kernel, n, boards, rows, hands, leaf_count),
            out_shape=pltpu.VMEM((2, leaf_rows, hands), F32),
            in_specs=[pl.BlockSpec(memory_space=pl.ANY)] * len(arrays),
            out_specs=vmem,
            scratch_shapes=[
                pltpu.VMEM(chance_reach.shape, F32),
                pltpu.VMEM(regrets_start.shape, F32),
                pltpu.VMEM((1, leaf_rows), F32),
                pltpu.VMEM((2, 1, leaf_count), jnp.int32),
                pltpu.VMEM((2, hands), jnp.int32),
                pltpu.VMEM(board_cards.shape, jnp.int32),
                pltpu.VMEM(hand_rank.shape, jnp.int32),
                dma((len(arrays),)),
                pltpu.VMEM((round_up(near, 8), width), F32),
                pltpu.VMEM((near, width), F32),
                pltpu.VMEM((2, width), jnp.int32),
                pltpu.VMEM((round_up(boards, 8), width), jnp.int32),
                pltpu.VMEM((1, 2 * width + LANES), F32),
                pltpu.VMEM((1, 2 * width + LANES), F32),
                pltpu.VMEM((span, LANES), F32),
                pltpu.VMEM((2 * span, LANES), F32),
                pltpu.VMEM((2, total, hands), F32),
                pltpu.VMEM((2, span, hands), F32),
                pltpu.VMEM((ITERS, 2, total, hands), F32),
                pltpu.VMEM((ITERS, 2, total, hands), F32),
                pltpu.VMEM((2, 2 * rows, hands), F32),
                pltpu.VMEM((2, total, hands), F32),
                pltpu.VMEM((ITERS, 2, LANES), F32),
                pltpu.VMEM((ITERS, 2 * n - 1, 2, LANES), F32),
                pltpu.VMEM((edged, hands), F32),
                pltpu.VMEM((leaf_rows, hands), F32),
                pltpu.VMEM((edged, hands), F32),
                pltpu.VMEM((2, span, hands), F32),
                pltpu.VMEM((2, 1, hands), F32),
                pltpu.VMEM((1, hands), F32),
                pltpu.VMEM((2, rows, hands), F32),
                pltpu.VMEM((rows, hands), F32),
                pltpu.VMEM((2, rows, hands), F32),
                pltpu.VMEM((2, 2 * rows, hands), F32),
                pltpu.SemaphoreType.REGULAR,
                dma((PUTS,)), dma((GETS,)),
                dma((ITERS,)), dma((ITERS,)),
            ],
            compiler_params=pltpu.CompilerParams(collective_id=0, has_side_effects=True),
            name="regret",
        )(*arrays)
        return outs[:1], outs[1:]

    in_specs = (
        P("player", "leaf", None),
        P("player", "leaf", None),
        P("leaf"),
        P("player", None),
        P(),
        P("leaf", None),
        P("leaf", None),
    )
    out_specs = (P("player", "leaf", None), P("player", "leaf", None))
    return jax.shard_map(local, mesh=mesh, in_specs=in_specs, out_specs=out_specs, check_vma=False)
```

```python
import functools

import jax
import jax.numpy as jnp
from jax import lax
from jax.experimental import pallas as pl
from jax.experimental.pallas import tpu as pltpu
from jax.sharding import PartitionSpec as P

ITERS = 2
MOST = 6
DELTA = 0.05
EPSILON = 1e-06
DECK_SIZE = 52
LANES = 128
WIDE = 256
PARTS = 1
MESH = pl.DeviceIdType.MESH
F32 = jnp.float32
BF16 = jnp.bfloat16
F8 = jnp.float8_e4m3fn

(GET_HALF, GET_BEHIND, GET_NEXT, GET_AHEAD, GET_LATE, GET_AFTER, GET_BEYOND, GET_CHANCE, GET_CHANCE_AFTER, GET_PARENT,
 GET_INFO, GET_LOW, GET_HIGH, GET_HIGHER, GET_VALUES, GET_EDGE_LOW, GET_EDGE_HIGH, GET_POLICY, GET_REGRETS, GETS) = (
    0, 1, 3, 5, 7, 9, 11, 13, 14, 16, 17, 18, 19, 20, 21, 22, 23, 24, 25, 26)
(PUT_HALF, PUT_BEHIND, PUT_NEXT, PUT_AHEAD, PUT_LATE, PUT_AFTER, PUT_BEYOND, PUT_CHANCE, PUT_CHANCE_BEFORE, PUT_PARENT,
 PUT_INFO, PUT_HIGH, PUT_LOW, PUT_LOWER, PUT_VALUES, PUT_EDGE, PUT_POLICY, PUT_REGRETS, PUTS) = (
    0, 1, 2, 3, 4, 5, 6, 7, 8, 9, 10, 11, 12, 13, 14, 15, 17, 18, 19)


def round_up(value, unit):
    return (value + unit - 1) // unit * unit


def row_of(column, count):
    down = lax.broadcasted_iota(jnp.int32, (count, count), 0)
    across = lax.broadcasted_iota(jnp.int32, (count, count), 1)
    return jnp.sum(jnp.where(down == across, column, 0.0), axis=0, keepdims=True)


def same_of(ids):
    twice = jnp.concatenate([ids, ids], axis=0)
    return (ids == row_of(twice, twice.shape[0])).astype(BF16)


def node_totals(same, array):
    coarse = array.astype(BF16)
    fine = (array - coarse.astype(F32)).astype(BF16)
    return jnp.dot(same, jnp.concatenate([coarse, fine], axis=0), preferred_element_type=F32)


def settle(view, semaphore):
    pltpu.make_async_copy(view, view, semaphore).wait()


def body(
    n, boards, rows, hands, leaf_count,
    chance_far, regrets_far, pot_far, parent_far, cards_far, board_cards_far, rank_far,
    outs,
    chance, regrets, pot, parents, cards, board_cards, rank, load,
    codes, free, cards_wide, rank_wide, info, info_in, pots, weight,
    held, chances, policy, values, landed, standing_one, square_out, square_in,
    last_policy, last_regrets, last_values, reach, behind, behind_out, ahead, ahead_out, late_before, late_after,
    all_in, put, get, square_send, square_recv,
    payoff, apart, turned, lows, right, same, same_own, same_last, split,
):
    me = lax.axis_index("leaf")
    player = lax.axis_index("player")
    other = 1 - player
    spot = 2 * me + player
    hub = 2 * n - 1
    width = free.shape[1]
    depth = right.shape[0]
    half = boards // 2
    near = half + 1
    local = boards * rows
    own = half * rows
    span = near * rows
    total = own + 3 * rows
    edge = min(MOST - 1, rows)
    rest = 2 * edge - rows
    last = ITERS - 1
    partner = {"player": other}

    def push(source, target, device, sent, received):
        pltpu.make_async_remote_copy(
            src_ref=source, dst_ref=target, send_sem=put.at[sent], recv_sem=get.at[received],
            device_id=device, device_id_type=MESH).start()

    def device_at(at):
        return {"leaf": at // 2, "player": at % 2}

    loads = [
        pltpu.make_async_copy(far, near_ref, load.at[i])
        for i, (far, near_ref) in enumerate((
            (cards_far, cards), (board_cards_far, board_cards), (rank_far, rank), (pot_far, pot), (regrets_far, regrets),
            (parent_far, parents.at[player]), (chance_far, chance)))]
    for copy in loads:
        copy.start()

    for p in range(2):
        held[p, :rows] = jnp.zeros((rows, hands), F32)
        held[p, rows + own :] = jnp.zeros((2 * rows, hands), F32)
        chances[p, own:] = jnp.zeros((rows, hands), F32)
        values[0, p, :rows] = jnp.zeros((rows, hands), F32)
        landed[p] = jnp.zeros((2 * rows, hands), F32)
        behind[p] = jnp.zeros((1, hands), F32)
        ahead[p] = jnp.zeros((rows, hands), F32)
        late_before[p] = jnp.zeros((rows, hands), F32)
        late_after[p] = jnp.zeros((2 * rows, hands), F32)
    last_values[:rows] = jnp.zeros((rows, hands), F32)
    last_values[rows + local :] = jnp.zeros((rows, hands), F32)

    barrier = pltpu.get_barrier_semaphore()

    def greet(device):
        pl.semaphore_signal(barrier, inc=1, device_id=device, device_id_type=MESH)

    greet(partner)

    @pl.when((player == 0) & (me > 0))
    def _():
        for p in range(2):
            greet({"leaf": me - 1, "player": p})

    @pl.when((player == 1) & (me < n - 1))
    def _():
        for p in range(2):
            greet({"leaf": me + 1, "player": p})

    @pl.when(spot < hub - 2)
    def _():
        greet({"leaf": n - 1, "player": 1})

    for copy in loads[:4]:
        copy.wait()

    cards_wide[...] = jnp.full(cards_wide.shape, -1, jnp.int32)
    cards_wide[:, :hands] = cards[...]
    rank_wide[...] = jnp.zeros(rank_wide.shape, jnp.int32)
    rank_wide[:boards, :hands] = rank[...]
    card = lax.broadcasted_iota(jnp.int32, (depth, width), 0)
    lane = lax.broadcasted_iota(jnp.int32, (depth, width), 1)
    holding = ((card == cards_wide[0:1, :]) | (card == cards_wide[1:2, :])).astype(F32)
    valid = ((card == depth - 1) & (lane < hands)).astype(F32)
    ranked = rank_wide[...]
    code = ((128 + (ranked & 127)) << (ranked >> 7)).astype(F32)
    deck = lax.broadcasted_iota(jnp.int32, (boards, depth), 1)
    on_board = jnp.zeros((boards, depth), jnp.bool_)
    for k in range(board_cards.shape[1]):
        on_board = on_board | (deck == board_cards[:, k : k + 1])
    touched = jnp.dot(on_board.astype(BF16), holding.astype(BF16), preferred_element_type=F32)
    untouched = (touched < 0.5).astype(F32)
    first = player == 0
    turned[...] = (holding + valid).T.astype(F8)
    codes[...] = jnp.zeros(codes.shape, F32)
    codes[:half] = jnp.where(first, code[:half], code[half:boards])
    codes[half:near] = code[half : half + 1]
    free[:half] = jnp.where(first, untouched[:half], untouched[half:])
    free[half:near] = untouched[half : half + 1]
    right[...] = (valid - holding).astype(F8)
    info[...] = jnp.zeros(info.shape, F32)
    info[:, :width] = code[:1]
    info[:, width : 2 * width] = untouched[:1]
    info[:, 2 * width : 2 * width + local] = pot[...]
    down = lax.broadcasted_iota(jnp.int32, (span, local), 0)
    across = lax.broadcasted_iota(jnp.int32, (span, local), 1)
    pots[...] = jnp.broadcast_to(
        jnp.sum(jnp.where(across == down + player * own, pot[...] * (1.0 / hands), 0.0), axis=1, keepdims=True),
        (span, LANES))
    split[...] = jnp.zeros(split.shape, BF16)

    blocks = width // LANES
    length = width // PARTS

    def separate(first, last):
        for c in range(first, last, 2):
            found = jnp.dot(
                turned[...], right[:, c * LANES : min(c + 2, blocks) * LANES], preferred_element_type=F32).astype(BF16)
            for k in range(min(2, blocks - c)):
                apart[c + k] = found[:, k * LANES : (k + 1) * LANES].reshape(PARTS, length, LANES)

    def lower(begin, count):
        columns = codes[...].T
        for b in range(count):
            lows[b] = jnp.broadcast_to(
                columns[:, begin + b : begin + b + 1], (width, LANES)).astype(BF16).reshape(PARTS, length, LANES)

    def build(begin, count):
        def column(c, carry):
            at = pl.multiple_of(c * LANES, LANES)
            highs = [
                jnp.broadcast_to(
                    codes[begin + b : begin + b + 1, pl.ds(at, LANES)], (32, LANES)).astype(BF16)
                for b in range(count)]

            def part(k, carry):
                for r in range(0, length, 32):
                    bound = apart[c, k, r : r + 32]
                    floor = -bound
                    for b in range(count):
                        gap = highs[b] - lows[b, k, r : r + 32]
                        payoff[begin + b, c, k, r : r + 32] = jnp.minimum(jnp.maximum(gap, floor), bound).astype(F8)
                return carry

            return lax.fori_loop(0, PARTS, part, carry)

        return column

    for copy in loads[4:]:
        copy.wait()

    def ids_of(p, begin, count):
        leaf = begin + lax.broadcasted_iota(jnp.int32, (count, leaf_count), 0)
        here = lax.broadcasted_iota(jnp.int32, (count, leaf_count), 1)
        return jnp.sum(jnp.where(leaf == here, parents[p].astype(F32) + 1.0, 0.0), axis=1, keepdims=True)

    found = ids_of(player, me * local - rows, 3 * rows)
    positive = jnp.maximum(regrets[0, : 2 * rows], 0.0) + DELTA
    shared = (found[rows : 2 * rows] == found[rows - 1 : rows]) & (found[rows - 1 : rows] > 0.0)
    partial = node_totals(same_of(found[rows:]), positive)[:rows]
    ahead_out[...] = chance[0, :rows] * positive[:rows] / jnp.where(shared, 1.0, partial)
    found = ids_of(player, (me + 1) * local - rows, rows)
    positive = jnp.maximum(regrets[0, local - rows :], 0.0) + DELTA
    behind_out[...] = jnp.sum(jnp.where(found == found[rows - 1 :], positive, 0.0), axis=0, keepdims=True)

    @pl.when(me == 0)
    def _():
        separate(0, blocks)

    @pl.when(spot < hub)
    def _():
        pl.semaphore_wait(barrier, 1 + (me > 0).astype(jnp.int32) + (me < n - 1).astype(jnp.int32))

    @pl.when(spot == hub)
    def _():
        pl.semaphore_wait(barrier, 2 * n - 1)

    @pl.when((player == 1) & (me > 0))
    def _():
        push(info, info_in, {"leaf": me - 1, "player": 1}, PUT_INFO, GET_INFO)

    @pl.when(me < n - 1)
    def _():
        push(behind_out, behind.at[player], {"leaf": me + 1, "player": 0}, PUT_BEHIND, GET_BEHIND + player)

    @pl.when(me > 0)
    def _():
        to = {"leaf": me - 1, "player": 1}
        push(regrets.at[0, pl.ds(0, edge)], held.at[player, pl.ds(rows + own, edge)], to, PUT_NEXT, GET_NEXT + player)
        push(ahead_out.at[pl.ds(0, edge)], ahead.at[player, pl.ds(0, edge)], to, PUT_AHEAD, GET_AHEAD + player)

    push(parents.at[player], parents.at[player], partner, PUT_PARENT, GET_PARENT)

    @pl.when(player == 0)
    def _():
        push(regrets.at[0, pl.ds(own - rows, own + rows)], held.at[0, pl.ds(0, own + rows)], partner, PUT_HALF, GET_HALF)
        push(chance.at[0, pl.ds(own, own)], chances.at[0, pl.ds(0, own)], partner, PUT_CHANCE, GET_CHANCE)
        held[0, rows:] = regrets[0, : own + 2 * rows]
        chances[0] = chance[0, :span]

    @pl.when(player == 1)
    def _():
        push(regrets.at[0, pl.ds(0, own + 2 * rows)], held.at[1, pl.ds(rows, own + 2 * rows)], partner, PUT_HALF, GET_HALF)
        push(chance.at[0, pl.ds(0, span)], chances.at[1], partner, PUT_CHANCE, GET_CHANCE)
        held[1, : own + rows] = regrets[0, own - rows :]
        chances[1, :own] = chance[0, own:]

    @pl.when(spot == hub)
    def _():
        def welcome(k, carry):
            pl.semaphore_signal(
                all_in, inc=1, device_id=k - 1, device_id_type=pl.DeviceIdType.LOGICAL)
            return carry

        lax.fori_loop(1, 2 * n, welcome, 0)

    @pl.when(me > 0)
    def _():
        separate(0, blocks)

    lower(0, half)
    lax.fori_loop(0, blocks, build(0, half), 0)

    @pl.when(me < n - 1)
    def _():
        push(
            regrets.at[0, pl.ds(local - edge, edge)], late_before.at[player, pl.ds(rows - edge, edge)],
            {"leaf": me + 1, "player": 0}, PUT_LATE, GET_LATE + player)

    @pl.when(me > 0)
    def _():
        to = {"leaf": me - 1, "player": 1}
        push(
            regrets.at[0, pl.ds(edge, rows - edge)], late_after.at[player, pl.ds(edge, rows - edge)], to, PUT_AFTER,
            GET_AFTER + player)
        push(
            regrets.at[0, pl.ds(rows, rest)], late_after.at[player, pl.ds(rows, rest)], to, PUT_BEYOND,
            GET_BEYOND + player)

    settle(parents.at[other], get.at[GET_PARENT])

    ids = []
    weights = []
    order = lax.broadcasted_iota(jnp.int32, (span, 1), 0)
    for p in range(2):
        found = ids_of(p, spot * own - rows, total)
        found = jnp.where(found > 0.0, found + p * (leaf_count + 1.0), 0.0)
        inside = found[rows : rows + span]
        counted = (inside > 0.0) & (inside != found[rows - 1 : rows])
        counted = counted & ((order < own) | (inside == found[rows + own - 1 : rows + own]))
        ids.append(found)
        weights.append(counted.astype(F32))
    same[...] = same_of(jnp.concatenate(ids, axis=0))
    same_own[...] = same_of(jnp.concatenate([found[rows : rows + span] for found in ids], axis=0))
    weight[...] = jnp.broadcast_to(jnp.concatenate(weights, axis=0), (2 * span, LANES))

    @pl.when((player == 1) & (me < n - 1))
    def _():
        settle(info_in, get.at[GET_INFO])
        codes[half:near] = info_in[:, :width]
        free[half:near] = info_in[:, width : 2 * width]
        pots[own:] = jnp.broadcast_to(
            jnp.sum(
                jnp.where(across[:rows] == down[:rows], info_in[:, 2 * width : 2 * width + local] * (1.0 / hands), 0.0),
                axis=1, keepdims=True),
            (rows, LANES))

    lower(half, 1)
    lax.fori_loop(0, blocks, build(half, 1), 0)

    @pl.when((player == 0) & (me > 0))
    def _():
        for p in range(2):
            settle(behind.at[p], get.at[GET_BEHIND + p])

    @pl.when((player == 1) & (me < n - 1))
    def _():
        for p in range(2):
            settle(held.at[p, pl.ds(rows + own, edge)], get.at[GET_NEXT + p])
            settle(ahead.at[p, pl.ds(0, edge)], get.at[GET_AHEAD + p])

    @pl.when(player == 0)
    def _():
        settle(held.at[1, pl.ds(rows, own + 2 * rows)], get.at[GET_HALF])
        settle(chances.at[1], get.at[GET_CHANCE])

    @pl.when(player == 1)
    def _():
        settle(held.at[0, pl.ds(0, own + rows)], get.at[GET_HALF])
        settle(chances.at[0, pl.ds(0, own)], get.at[GET_CHANCE])

    def strategy(standing):
        positive = jnp.maximum(standing, 0.0) + DELTA
        return positive / node_totals(same[...], positive)

    for it in range(ITERS):
        if it == 0:
            at = lax.broadcasted_iota(jnp.int32, (2 * total, 1), 0)
            at = jnp.where(at >= total, at - total, at)
            present = ((player == 0) & (at >= rows)) | ((player == 1) & (at < rows + own + edge))
            positive = jnp.where(present, jnp.maximum(held[...].reshape(2 * total, hands), 0.0) + DELTA, 0.0)
            totals = node_totals(same[...], positive)
            for p in range(2):
                found = ids[p]
                mine = slice(p * total + rows, p * total + rows + own)
                beside = slice(mine.stop, mine.stop + rows)
                back = (found[rows : rows + own] == found[rows - 1 : rows]) & (found[rows - 1 : rows] > 0.0)
                forth = found[rows + own : rows + span] == found[rows + own - 1 : rows + own]
                choice = positive[mine] / (totals[mine] + jnp.where(back, behind[p], 0.0))
                policy[0, p, rows : rows + own] = choice
                reach[p, :own] = chances[p, :own] * choice
                policy[0, p, rows + own : rows + span] = positive[beside] / jnp.where(forth, totals[beside], 1.0)
                reach[p, own:] = jnp.where(player == 0, chances[p, own:] * positive[beside], ahead[p]) / jnp.where(
                    forth | (player == 0), totals[beside], 1.0)
        else:
            policy[it] = strategy(standing).reshape(2, total, hands)
            for p in range(2):
                reach[p, :own] = chances[p, :own] * policy[it, p, rows : rows + own]
                reach[p, own:] = chances[p, own:] * policy[it, p, rows + own : rows + span]
        if it == last:
            standing_one[...] = standing.reshape(2, total, hands)
            push(
                policy.at[it, other, pl.ds(pl.multiple_of(player * rows, rows), span)],
                last_policy.at[pl.ds(pl.multiple_of(player * span, rows), span)], partner, PUT_POLICY, GET_POLICY)
            push(
                standing_one.at[other, pl.ds(rows, own)], last_regrets.at[pl.ds(pl.multiple_of(player * own, rows), own)],
                partner, PUT_REGRETS, GET_REGRETS)

        for b in range(near):
            seen = slice(b * rows, (b + 1) * rows)
            kept = slice((b + 1) * rows, (b + 2) * rows)
            open_hands = free[b : b + 1, :]
            facing = jnp.concatenate([reach[p, seen] for p in range(2)], axis=0)
            facing = facing * open_hands[:, :hands]
            coarse = facing.astype(BF16).astype(F32)
            split[b, :, :hands] = jnp.concatenate([coarse, facing - coarse], axis=0).astype(BF16)
            summed = jnp.concatenate([
                jnp.dot(
                    split[b],
                    jnp.concatenate([payoff[b, k].reshape(width, LANES) for k in range(c, min(c + 2, blocks))], axis=1),
                    preferred_element_type=F32)
                for c in range(0, blocks, 2)], axis=1)
            stake = jnp.concatenate([pots[seen, :1]] * 2, axis=0)
            summed = (summed[: 2 * rows] + summed[2 * rows :])[:, :hands] + facing
            summed = summed * open_hands[:, :hands] * stake
            values[it, 1, kept] = summed[:rows]
            values[it, 0, kept] = summed[rows:]
            if b == 0 and it < last:
                @pl.when(spot > 0)
                def _(it=it):
                    push(
                        values.at[it, :, pl.ds(rows + edge, rows - edge)], landed.at[:, pl.ds(edge, rows - edge)],
                        device_at(spot - 1), PUT_LOW, GET_HIGH)

            if b == half - 1 and it < last:
                @pl.when(spot < hub)
                def _(it=it):
                    push(
                        values.at[it, :, pl.ds(rows + own - edge, edge)], values.at[it, :, pl.ds(rows - edge, edge)],
                        device_at(spot + 1), PUT_HIGH, GET_LOW)

                @pl.when(spot > 0)
                def _(it=it):
                    push(
                        values.at[it, :, pl.ds(2 * rows, rest)], landed.at[:, pl.ds(rows, rest)],
                        device_at(spot - 1), PUT_LOWER, GET_HIGHER)
            if b == half - 1 and it == last:
                push(
                    values.at[it, other, pl.ds(rows, own)],
                    last_values.at[pl.ds(pl.multiple_of(rows + player * own, rows), own)], partner, PUT_VALUES, GET_VALUES)

                @pl.when((player == 1) & (me < n - 1))
                def _(it=it):
                    for p in range(2):
                        push(
                            values.at[it, p, pl.ds(rows + own - edge, edge)], last_values.at[pl.ds(rows - edge, edge)],
                            {"leaf": me + 1, "player": p}, PUT_EDGE + p, GET_EDGE_LOW)

                @pl.when((player == 0) & (me > 0))
                def _(it=it):
                    for p in range(2):
                        push(
                            values.at[it, p, pl.ds(rows, edge)], last_values.at[pl.ds(rows + local, edge)],
                            {"leaf": me - 1, "player": p}, PUT_EDGE + p, GET_EDGE_HIGH)

        gained = jnp.concatenate([values[it, p, rows : rows + span] for p in range(2)], axis=0)
        played = jnp.concatenate([policy[it, p, rows : rows + span] for p in range(2)], axis=0)
        instant = (gained - node_totals(same_own[...], played * gained)) * weight[:, :1]
        squares = jnp.sum((instant * instant).reshape(2, span, hands), axis=1)
        square_out[it] = jnp.broadcast_to(jnp.sum(squares, axis=1, keepdims=True), (2, LANES))

        if it == 0:
            @pl.when(spot < hub)
            def _():
                pl.semaphore_wait(all_in, 1)

        def tell(t, carry, it=it):
            at = t if it == last else jnp.where(spot < n, 2 * n - 2 - t, t)
            ahead = (at >= spot).astype(jnp.int32)
            pltpu.make_async_remote_copy(
                src_ref=square_out.at[it], dst_ref=square_in.at[it, spot - 1 + ahead],
                send_sem=square_send.at[it], recv_sem=square_recv.at[it],
                device_id=at + ahead, device_id_type=pl.DeviceIdType.LOGICAL).start()
            return carry

        lax.fori_loop(0, 2 * n - 1, tell, 0)

        if it == 0:
            same_last[...] = same_of(ids_of(player, me * local - rows, local + 2 * rows))
            @pl.when((player == 0) & (me > 0))
            def _():
                for p in range(2):
                    settle(late_before.at[p, pl.ds(rows - edge, edge)], get.at[GET_LATE + p])

            @pl.when((player == 1) & (me < n - 1))
            def _():
                for p in range(2):
                    settle(late_after.at[p, pl.ds(edge, rows - edge)], get.at[GET_AFTER + p])
                    settle(late_after.at[p, pl.ds(rows, rest)], get.at[GET_BEYOND + p])

            standing = jnp.concatenate([
                part for p in range(2) for part in (
                    held[p, :rows] + late_before[p], held[p, rows : rows + own],
                    held[p, rows + own :] + late_after[p])], axis=0)
            policy[0] = strategy(standing).reshape(2, total, hands)
            for p in range(2):
                beside = slice(p * total + rows + own, p * total + rows + span)
                forth = ids[p][rows + own : rows + span] == ids[p][rows + own - 1 : rows + own]
                factor = jnp.where(forth, jnp.maximum(standing[beside], 0.0) + DELTA, policy[0, p, rows + own : rows + span])
                chances[p, own:] = jnp.where(player == 0, chances[p, own:], ahead[p] / factor)

        if it < last:
            @pl.when(spot > 0)
            def _(it=it):
                settle(values.at[it, :, pl.ds(rows - edge, edge)], get.at[GET_LOW])

            @pl.when(spot < hub)
            def _():
                settle(landed.at[:, pl.ds(edge, rows - edge)], get.at[GET_HIGH])
                settle(landed.at[:, pl.ds(rows, rest)], get.at[GET_HIGHER])

            inner = lax.broadcasted_iota(jnp.int32, (rows, hands), 0) < edge
            gained = jnp.concatenate([
                part for p in range(2) for part in (
                    values[it, p, : rows + own], jnp.where(inner, values[it, p, rows + own : rows + span], landed[p, :rows]),
                    landed[p, rows:])], axis=0)
            instant = gained - node_totals(same[...], policy[it].reshape(2 * total, hands) * gained)
        else:
            mine = pl.ds(pl.multiple_of(player * span, rows), span)
            last_policy[mine] = policy[it, player, pl.ds(pl.multiple_of(player * rows, rows), span)]
            last_regrets[pl.ds(pl.multiple_of(player * own, rows), own)] = standing_one[player, pl.ds(rows, own)]
            last_values[pl.ds(pl.multiple_of(rows + player * own, rows), own)] = values[it, player, pl.ds(rows, own)]
            settle(last_policy.at[pl.ds(pl.multiple_of(other * span, rows), span)], get.at[GET_POLICY])
            settle(last_regrets.at[pl.ds(pl.multiple_of(other * own, rows), own)], get.at[GET_REGRETS])
            settle(last_values.at[pl.ds(pl.multiple_of(rows + other * own, rows), own)], get.at[GET_VALUES])

            @pl.when(me > 0)
            def _():
                settle(last_values.at[pl.ds(rows - edge, edge)], get.at[GET_EDGE_LOW])

            @pl.when(me < n - 1)
            def _():
                settle(last_values.at[pl.ds(rows + local, edge)], get.at[GET_EDGE_HIGH])

            gained = last_values[...]
            instant = (gained - node_totals(same_last[...], last_policy[...] * gained))[rows : rows + local]
            outs[1] = gained[rows : rows + local]

        everyone = square_in.at[it]
        settle(everyone, square_recv.at[it])

        squares = square_out[it] + jnp.sum(square_in[it], axis=0)
        inverse = 1.0 / jnp.sqrt(squares / (leaf_count * hands) + EPSILON)
        if it < last:
            turn = lax.broadcasted_iota(jnp.int32, (2 * total, 1), 0) < total
            standing = standing + instant * jnp.where(turn, inverse[0:1, :1], inverse[1:2, :1])
        else:
            outs[0] = last_regrets[...] + instant * jnp.where(player == 0, inverse[0:1, :1], inverse[1:2, :1])

    def sent(view, slot):
        settle(view, put.at[slot])

    @pl.when(me > 0)
    def _():
        @pl.when(player == 1)
        def _():
            sent(info, PUT_INFO)

        sent(regrets.at[0, pl.ds(0, edge)], PUT_NEXT)
        sent(ahead_out.at[pl.ds(0, edge)], PUT_AHEAD)
        sent(regrets.at[0, pl.ds(edge, rows - edge)], PUT_AFTER)
        sent(regrets.at[0, pl.ds(rows, rest)], PUT_BEYOND)

    @pl.when(me < n - 1)
    def _():
        sent(behind_out, PUT_BEHIND)
        sent(regrets.at[0, pl.ds(local - edge, edge)], PUT_LATE)

    sent(parents.at[player], PUT_PARENT)

    @pl.when(player == 0)
    def _():
        sent(regrets.at[0, pl.ds(own - rows, own + rows)], PUT_HALF)
        sent(chance.at[0, pl.ds(own, own)], PUT_CHANCE)

    @pl.when(player == 1)
    def _():
        sent(regrets.at[0, pl.ds(0, own + 2 * rows)], PUT_HALF)
        sent(chance.at[0, pl.ds(0, span)], PUT_CHANCE)

    for it in range(last):
        @pl.when(spot < hub)
        def _(it=it):
            sent(values.at[it, :, pl.ds(rows + own - edge, edge)], PUT_HIGH)

        @pl.when(spot > 0)
        def _(it=it):
            sent(values.at[it, :, pl.ds(rows + edge, rows - edge)], PUT_LOW)
            sent(values.at[it, :, pl.ds(2 * rows, rest)], PUT_LOWER)

    sent(policy.at[last, other, pl.ds(pl.multiple_of(player * rows, rows), span)], PUT_POLICY)
    sent(standing_one.at[other, pl.ds(rows, own)], PUT_REGRETS)
    sent(values.at[last, other, pl.ds(rows, own)], PUT_VALUES)

    @pl.when((player == 1) & (me < n - 1))
    def _():
        for p in range(2):
            sent(values.at[last, p, pl.ds(rows + own - edge, edge)], PUT_EDGE + p)

    @pl.when((player == 0) & (me > 0))
    def _():
        for p in range(2):
            sent(values.at[last, p, pl.ds(rows, edge)], PUT_EDGE + p)

    for it in range(ITERS):
        everyone = square_in.at[it]
        settle(everyone, square_send.at[it])


def kernel(n, boards, rows, hands, leaf_count, *refs):
    near = boards // 2 + 1
    span = near * rows
    total = span + 2 * rows
    edged = (boards + 2) * rows
    width = round_up(hands, LANES)
    depth = round_up(DECK_SIZE + 1, 32)
    pl.run_scoped(
        functools.partial(body, n, boards, rows, hands, leaf_count, *refs),
        pltpu.VMEM((near, width // LANES, PARTS, width // PARTS, LANES), F8),
        pltpu.VMEM((width // LANES, PARTS, width // PARTS, LANES), BF16),
        pltpu.VMEM((width, depth), F8),
        pltpu.VMEM((near, PARTS, width // PARTS, LANES), BF16),
        pltpu.VMEM((depth, width), F8),
        pltpu.VMEM((2 * total, 4 * total), BF16),
        pltpu.VMEM((2 * span, 4 * span), BF16),
        pltpu.VMEM((edged, 2 * edged), BF16),
        pltpu.VMEM((near, 4 * rows, width), BF16),
    )


def solution(mesh):
    n = mesh.shape["leaf"]

    def local(chance_reach, regrets_start, pot, parent, hand_cards, board_cards, hand_rank):
        leaf_rows, hands = chance_reach.shape[1:]
        boards = hand_rank.shape[0]
        rows = leaf_rows // boards
        leaf_count = parent.shape[1]
        width = round_up(hands, LANES)
        half = boards // 2
        near = half + 1
        span = near * rows
        total = (half + 3) * rows
        edged = leaf_rows + 2 * rows
        vmem = pl.BlockSpec(memory_space=pltpu.VMEM)
        shape = pltpu.VMEM(chance_reach.shape, F32)
        dma = pltpu.SemaphoreType.DMA
        arrays = (chance_reach, regrets_start, pot[None], parent, hand_cards.T, board_cards, hand_rank)
        outs = pl.pallas_call(
            functools.partial(kernel, n, boards, rows, hands, leaf_count),
            out_shape=pltpu.VMEM((2, leaf_rows, hands), F32),
            in_specs=[pl.BlockSpec(memory_space=pl.ANY)] * len(arrays),
            out_specs=vmem,
            scratch_shapes=[
                pltpu.VMEM(chance_reach.shape, F32),
                pltpu.VMEM(regrets_start.shape, F32),
                pltpu.VMEM((1, leaf_rows), F32),
                pltpu.VMEM((2, 1, leaf_count), jnp.int32),
                pltpu.VMEM((2, hands), jnp.int32),
                pltpu.VMEM(board_cards.shape, jnp.int32),
                pltpu.VMEM(hand_rank.shape, jnp.int32),
                dma((len(arrays),)),
                pltpu.VMEM((round_up(near, 8), width), F32),
                pltpu.VMEM((near, width), F32),
                pltpu.VMEM((2, width), jnp.int32),
                pltpu.VMEM((round_up(boards, 8), width), jnp.int32),
                pltpu.VMEM((1, 2 * width + LANES), F32),
                pltpu.VMEM((1, 2 * width + LANES), F32),
                pltpu.VMEM((span, LANES), F32),
                pltpu.VMEM((2 * span, LANES), F32),
                pltpu.VMEM((2, total, hands), F32),
                pltpu.VMEM((2, span, hands), F32),
                pltpu.VMEM((ITERS, 2, total, hands), F32),
                pltpu.VMEM((ITERS, 2, total, hands), F32),
                pltpu.VMEM((2, 2 * rows, hands), F32),
                pltpu.VMEM((2, total, hands), F32),
                pltpu.VMEM((ITERS, 2, LANES), F32),
                pltpu.VMEM((ITERS, 2 * n - 1, 2, LANES), F32),
                pltpu.VMEM((edged, hands), F32),
                pltpu.VMEM((leaf_rows, hands), F32),
                pltpu.VMEM((edged, hands), F32),
                pltpu.VMEM((2, span, hands), F32),
                pltpu.VMEM((2, 1, hands), F32),
                pltpu.VMEM((1, hands), F32),
                pltpu.VMEM((2, rows, hands), F32),
                pltpu.VMEM((rows, hands), F32),
                pltpu.VMEM((2, rows, hands), F32),
                pltpu.VMEM((2, 2 * rows, hands), F32),
                pltpu.SemaphoreType.REGULAR,
                dma((PUTS,)), dma((GETS,)),
                dma((ITERS,)), dma((ITERS,)),
            ],
            compiler_params=pltpu.CompilerParams(collective_id=0, has_side_effects=True),
            name="regret",
        )(*arrays)
        return outs[:1], outs[1:]

    in_specs = (
        P("player", "leaf", None),
        P("player", "leaf", None),
        P("leaf"),
        P("player", None),
        P(),
        P("leaf", None),
        P("leaf", None),
    )
    out_specs = (P("player", "leaf", None), P("player", "leaf", None))
    return jax.shard_map(local, mesh=mesh, in_specs=in_specs, out_specs=out_specs, check_vma=False)
```

```python
import functools

import jax
import jax.numpy as jnp
from jax import lax
from jax.experimental import pallas as pl
from jax.experimental.pallas import tpu as pltpu
from jax.sharding import PartitionSpec as P

ITERS = 2
MOST = 6
DELTA = 0.05
EPSILON = 1e-06
DECK_SIZE = 52
LANES = 128
WIDE = 256
PARTS = 1
MESH = pl.DeviceIdType.MESH
F32 = jnp.float32
BF16 = jnp.bfloat16
F8 = jnp.float8_e4m3fn

(GET_HALF, GET_BEHIND, GET_NEXT, GET_AHEAD, GET_LATE, GET_AFTER, GET_BEYOND, GET_CHANCE, GET_CHANCE_AFTER, GET_PARENT,
 GET_INFO, GET_LOW, GET_HIGH, GET_HIGHER, GET_VALUES, GET_EDGE_LOW, GET_EDGE_HIGH, GET_POLICY, GET_REGRETS, GETS) = (
    0, 1, 3, 5, 7, 9, 11, 13, 14, 16, 17, 18, 19, 20, 21, 22, 23, 24, 25, 26)
(PUT_HALF, PUT_BEHIND, PUT_NEXT, PUT_AHEAD, PUT_LATE, PUT_AFTER, PUT_BEYOND, PUT_CHANCE, PUT_CHANCE_BEFORE, PUT_PARENT,
 PUT_INFO, PUT_HIGH, PUT_LOW, PUT_LOWER, PUT_VALUES, PUT_EDGE, PUT_POLICY, PUT_REGRETS, PUTS) = (
    0, 1, 2, 3, 4, 5, 6, 7, 8, 9, 10, 11, 12, 13, 14, 15, 17, 18, 19)


def round_up(value, unit):
    return (value + unit - 1) // unit * unit


def row_of(column, count):
    down = lax.broadcasted_iota(jnp.int32, (count, count), 0)
    across = lax.broadcasted_iota(jnp.int32, (count, count), 1)
    return jnp.sum(jnp.where(down == across, column, 0.0), axis=0, keepdims=True)


def same_of(ids):
    twice = jnp.concatenate([ids, ids], axis=0)
    return (ids == row_of(twice, twice.shape[0])).astype(BF16)


def node_totals(same, array):
    coarse = array.astype(BF16)
    fine = (array - coarse.astype(F32)).astype(BF16)
    return jnp.dot(same, jnp.concatenate([coarse, fine], axis=0), preferred_element_type=F32)


def settle(view, semaphore):
    pltpu.make_async_copy(view, view, semaphore).wait()


def body(
    n, boards, rows, hands, leaf_count,
    chance_far, regrets_far, pot_far, parent_far, cards_far, board_cards_far, rank_far,
    outs,
    chance, regrets, pot, parents, cards, board_cards, rank, load,
    codes, free, cards_wide, rank_wide, info, info_in, pots, weight,
    held, chances, policy, values, landed, standing_one, square_out, square_in,
    last_policy, last_regrets, last_values, reach, behind, behind_out, ahead, ahead_out, late_before, late_after,
    all_in, put, get, square_send, square_recv,
    payoff, apart, turned, lows, right, same, same_own, same_last, split,
):
    me = lax.axis_index("leaf")
    player = lax.axis_index("player")
    other = 1 - player
    spot = 2 * me + player
    hub = 2 * n - 1
    width = free.shape[1]
    depth = right.shape[0]
    half = boards // 2
    near = half + 1
    local = boards * rows
    own = half * rows
    span = near * rows
    total = own + 3 * rows
    edge = min(MOST - 1, rows)
    rest = 2 * edge - rows
    last = ITERS - 1
    partner = {"player": other}

    def push(source, target, device, sent, received):
        pltpu.make_async_remote_copy(
            src_ref=source, dst_ref=target, send_sem=put.at[sent], recv_sem=get.at[received],
            device_id=device, device_id_type=MESH).start()

    def device_at(at):
        return {"leaf": at // 2, "player": at % 2}

    loads = [
        pltpu.make_async_copy(far, near_ref, load.at[i])
        for i, (far, near_ref) in enumerate((
            (cards_far, cards), (board_cards_far, board_cards), (rank_far, rank), (pot_far, pot), (regrets_far, regrets),
            (parent_far, parents.at[player]), (chance_far, chance)))]
    for copy in loads:
        copy.start()

    for p in range(2):
        held[p, :rows] = jnp.zeros((rows, hands), F32)
        held[p, rows + own :] = jnp.zeros((2 * rows, hands), F32)
        chances[p, own:] = jnp.zeros((rows, hands), F32)
        values[0, p, :rows] = jnp.zeros((rows, hands), F32)
        landed[p] = jnp.zeros((2 * rows, hands), F32)
        behind[p] = jnp.zeros((1, hands), F32)
        ahead[p] = jnp.zeros((rows, hands), F32)
        late_before[p] = jnp.zeros((rows, hands), F32)
        late_after[p] = jnp.zeros((2 * rows, hands), F32)
    last_values[:rows] = jnp.zeros((rows, hands), F32)
    last_values[rows + local :] = jnp.zeros((rows, hands), F32)

    barrier = pltpu.get_barrier_semaphore()

    def greet(device):
        pl.semaphore_signal(barrier, inc=1, device_id=device, device_id_type=MESH)

    greet(partner)

    @pl.when((player == 0) & (me > 0))
    def _():
        for p in range(2):
            greet({"leaf": me - 1, "player": p})

    @pl.when((player == 1) & (me < n - 1))
    def _():
        for p in range(2):
            greet({"leaf": me + 1, "player": p})

    @pl.when(spot < hub - 2)
    def _():
        greet({"leaf": n - 1, "player": 1})

    for copy in loads[:4]:
        copy.wait()

    cards_wide[...] = jnp.full(cards_wide.shape, -1, jnp.int32)
    cards_wide[:, :hands] = cards[...]
    rank_wide[...] = jnp.zeros(rank_wide.shape, jnp.int32)
    rank_wide[:boards, :hands] = rank[...]
    card = lax.broadcasted_iota(jnp.int32, (depth, width), 0)
    lane = lax.broadcasted_iota(jnp.int32, (depth, width), 1)
    holding = ((card == cards_wide[0:1, :]) | (card == cards_wide[1:2, :])).astype(F32)
    valid = ((card == depth - 1) & (lane < hands)).astype(F32)
    ranked = rank_wide[...]
    code = ((128 + (ranked & 127)) << (ranked >> 7)).astype(F32)
    deck = lax.broadcasted_iota(jnp.int32, (boards, depth), 1)
    on_board = jnp.zeros((boards, depth), jnp.bool_)
    for k in range(board_cards.shape[1]):
        on_board = on_board | (deck == board_cards[:, k : k + 1])
    touched = jnp.dot(on_board.astype(BF16), holding.astype(BF16), preferred_element_type=F32)
    untouched = (touched < 0.5).astype(F32)
    first = player == 0
    turned[...] = (holding + valid).T.astype(F8)
    codes[...] = jnp.zeros(codes.shape, F32)
    codes[:half] = jnp.where(first, code[:half], code[half:boards])
    codes[half:near] = code[half : half + 1]
    free[:half] = jnp.where(first, untouched[:half], untouched[half:])
    free[half:near] = untouched[half : half + 1]
    right[...] = (valid - holding).astype(F8)
    info[...] = jnp.zeros(info.shape, F32)
    info[:, :width] = code[:1]
    info[:, width : 2 * width] = untouched[:1]
    info[:, 2 * width : 2 * width + local] = pot[...]
    down = lax.broadcasted_iota(jnp.int32, (span, local), 0)
    across = lax.broadcasted_iota(jnp.int32, (span, local), 1)
    pots[...] = jnp.broadcast_to(
        jnp.sum(jnp.where(across == down + player * own, pot[...] * (1.0 / hands), 0.0), axis=1, keepdims=True),
        (span, LANES))
    split[...] = jnp.zeros(split.shape, BF16)

    blocks = width // LANES
    length = width // PARTS

    def separate(first, last):
        for c in range(first, last, 2):
            found = jnp.dot(
                turned[...], right[:, c * LANES : min(c + 2, blocks) * LANES], preferred_element_type=F32).astype(BF16)
            for k in range(min(2, blocks - c)):
                apart[c + k] = found[:, k * LANES : (k + 1) * LANES].reshape(PARTS, length, LANES)

    def lower(begin, count):
        columns = codes[...].T
        for b in range(count):
            lows[b] = jnp.broadcast_to(
                columns[:, begin + b : begin + b + 1], (width, LANES)).astype(BF16).reshape(PARTS, length, LANES)

    def build(begin, count):
        def column(c, carry):
            at = pl.multiple_of(c * LANES, LANES)
            highs = [
                jnp.broadcast_to(
                    codes[begin + b : begin + b + 1, pl.ds(at, LANES)], (32, LANES)).astype(BF16)
                for b in range(count)]

            def part(k, carry):
                for r in range(0, length, 32):
                    bound = apart[c, k, r : r + 32]
                    floor = -bound
                    for b in range(count):
                        gap = highs[b] - lows[b, k, r : r + 32]
                        payoff[begin + b, c, k, r : r + 32] = jnp.minimum(jnp.maximum(gap, floor), bound).astype(F8)
                return carry

            return lax.fori_loop(0, PARTS, part, carry)

        return column

    for copy in loads[4:]:
        copy.wait()

    def ids_of(p, begin, count):
        leaf = begin + lax.broadcasted_iota(jnp.int32, (count, leaf_count), 0)
        here = lax.broadcasted_iota(jnp.int32, (count, leaf_count), 1)
        return jnp.sum(jnp.where(leaf == here, parents[p].astype(F32) + 1.0, 0.0), axis=1, keepdims=True)

    found = ids_of(player, me * local - rows, 3 * rows)
    positive = jnp.maximum(regrets[0, : 2 * rows], 0.0) + DELTA
    shared = (found[rows : 2 * rows] == found[rows - 1 : rows]) & (found[rows - 1 : rows] > 0.0)
    partial = node_totals(same_of(found[rows:]), positive)[:rows]
    ahead_out[...] = chance[0, :rows] * positive[:rows] / jnp.where(shared, 1.0, partial)
    found = ids_of(player, (me + 1) * local - rows, rows)
    positive = jnp.maximum(regrets[0, local - rows :], 0.0) + DELTA
    behind_out[...] = jnp.sum(jnp.where(found == found[rows - 1 :], positive, 0.0), axis=0, keepdims=True)

    @pl.when(me == 0)
    def _():
        separate(0, blocks)

    @pl.when(spot < hub)
    def _():
        pl.semaphore_wait(barrier, 1 + (me > 0).astype(jnp.int32) + (me < n - 1).astype(jnp.int32))

    @pl.when(spot == hub)
    def _():
        pl.semaphore_wait(barrier, 2 * n - 1)

    @pl.when((player == 1) & (me > 0))
    def _():
        push(info, info_in, {"leaf": me - 1, "player": 1}, PUT_INFO, GET_INFO)

    @pl.when(me < n - 1)
    def _():
        push(behind_out, behind.at[player], {"leaf": me + 1, "player": 0}, PUT_BEHIND, GET_BEHIND + player)

    @pl.when(me > 0)
    def _():
        to = {"leaf": me - 1, "player": 1}
        push(regrets.at[0, pl.ds(0, edge)], held.at[player, pl.ds(rows + own, edge)], to, PUT_NEXT, GET_NEXT + player)
        push(ahead_out.at[pl.ds(0, edge)], ahead.at[player, pl.ds(0, edge)], to, PUT_AHEAD, GET_AHEAD + player)

    push(parents.at[player], parents.at[player], partner, PUT_PARENT, GET_PARENT)

    @pl.when(player == 0)
    def _():
        push(regrets.at[0, pl.ds(own - rows, own + rows)], held.at[0, pl.ds(0, own + rows)], partner, PUT_HALF, GET_HALF)
        push(chance.at[0, pl.ds(own, own)], chances.at[0, pl.ds(0, own)], partner, PUT_CHANCE, GET_CHANCE)
        held[0, rows:] = regrets[0, : own + 2 * rows]
        chances[0] = chance[0, :span]

    @pl.when(player == 1)
    def _():
        push(regrets.at[0, pl.ds(0, own + 2 * rows)], held.at[1, pl.ds(rows, own + 2 * rows)], partner, PUT_HALF, GET_HALF)
        push(chance.at[0, pl.ds(0, span)], chances.at[1], partner, PUT_CHANCE, GET_CHANCE)
        held[1, : own + rows] = regrets[0, own - rows :]
        chances[1, :own] = chance[0, own:]

    @pl.when(spot == hub)
    def _():
        def welcome(k, carry):
            pl.semaphore_signal(
                all_in, inc=1, device_id=k - 1, device_id_type=pl.DeviceIdType.LOGICAL)
            return carry

        lax.fori_loop(1, 2 * n, welcome, 0)

    @pl.when(me > 0)
    def _():
        separate(0, blocks)

    lower(0, half)
    lax.fori_loop(0, blocks, build(0, half), 0)

    @pl.when(me < n - 1)
    def _():
        push(
            regrets.at[0, pl.ds(local - edge, edge)], late_before.at[player, pl.ds(rows - edge, edge)],
            {"leaf": me + 1, "player": 0}, PUT_LATE, GET_LATE + player)

    @pl.when(me > 0)
    def _():
        to = {"leaf": me - 1, "player": 1}
        push(
            regrets.at[0, pl.ds(edge, rows - edge)], late_after.at[player, pl.ds(edge, rows - edge)], to, PUT_AFTER,
            GET_AFTER + player)
        push(
            regrets.at[0, pl.ds(rows, rest)], late_after.at[player, pl.ds(rows, rest)], to, PUT_BEYOND,
            GET_BEYOND + player)

    settle(parents.at[other], get.at[GET_PARENT])

    ids = []
    weights = []
    order = lax.broadcasted_iota(jnp.int32, (span, 1), 0)
    for p in range(2):
        found = ids_of(p, spot * own - rows, total)
        found = jnp.where(found > 0.0, found + p * (leaf_count + 1.0), 0.0)
        inside = found[rows : rows + span]
        counted = (inside > 0.0) & (inside != found[rows - 1 : rows])
        counted = counted & ((order < own) | (inside == found[rows + own - 1 : rows + own]))
        ids.append(found)
        weights.append(counted.astype(F32))
    same[...] = same_of(jnp.concatenate(ids, axis=0))
    same_own[...] = same_of(jnp.concatenate([found[rows : rows + span] for found in ids], axis=0))
    weight[...] = jnp.broadcast_to(jnp.concatenate(weights, axis=0), (2 * span, LANES))

    @pl.when((player == 1) & (me < n - 1))
    def _():
        settle(info_in, get.at[GET_INFO])
        codes[half:near] = info_in[:, :width]
        free[half:near] = info_in[:, width : 2 * width]
        pots[own:] = jnp.broadcast_to(
            jnp.sum(
                jnp.where(across[:rows] == down[:rows], info_in[:, 2 * width : 2 * width + local] * (1.0 / hands), 0.0),
                axis=1, keepdims=True),
            (rows, LANES))

    lower(half, 1)
    lax.fori_loop(0, blocks, build(half, 1), 0)

    @pl.when((player == 0) & (me > 0))
    def _():
        for p in range(2):
            settle(behind.at[p], get.at[GET_BEHIND + p])

    @pl.when((player == 1) & (me < n - 1))
    def _():
        for p in range(2):
            settle(held.at[p, pl.ds(rows + own, edge)], get.at[GET_NEXT + p])
            settle(ahead.at[p, pl.ds(0, edge)], get.at[GET_AHEAD + p])

    @pl.when(player == 0)
    def _():
        settle(held.at[1, pl.ds(rows, own + 2 * rows)], get.at[GET_HALF])
        settle(chances.at[1], get.at[GET_CHANCE])

    @pl.when(player == 1)
    def _():
        settle(held.at[0, pl.ds(0, own + rows)], get.at[GET_HALF])
        settle(chances.at[0, pl.ds(0, own)], get.at[GET_CHANCE])

    def strategy(standing):
        positive = jnp.maximum(standing, 0.0) + DELTA
        return positive / node_totals(same[...], positive)

    for it in range(ITERS):
        if it == 0:
            at = lax.broadcasted_iota(jnp.int32, (2 * total, 1), 0)
            at = jnp.where(at >= total, at - total, at)
            present = ((player == 0) & (at >= rows)) | ((player == 1) & (at < rows + own + edge))
            positive = jnp.where(present, jnp.maximum(held[...].reshape(2 * total, hands), 0.0) + DELTA, 0.0)
            totals = node_totals(same[...], positive)
            for p in range(2):
                found = ids[p]
                mine = slice(p * total + rows, p * total + rows + own)
                beside = slice(mine.stop, mine.stop + rows)
                back = (found[rows : rows + own] == found[rows - 1 : rows]) & (found[rows - 1 : rows] > 0.0)
                forth = found[rows + own : rows + span] == found[rows + own - 1 : rows + own]
                choice = positive[mine] / (totals[mine] + jnp.where(back, behind[p], 0.0))
                policy[0, p, rows : rows + own] = choice
                reach[p, :own] = chances[p, :own] * choice
                policy[0, p, rows + own : rows + span] = positive[beside] / jnp.where(forth, totals[beside], 1.0)
                reach[p, own:] = jnp.where(player == 0, chances[p, own:] * positive[beside], ahead[p]) / jnp.where(
                    forth | (player == 0), totals[beside], 1.0)
        else:
            policy[it] = strategy(standing).reshape(2, total, hands)
            for p in range(2):
                reach[p, :own] = chances[p, :own] * policy[it, p, rows : rows + own]
                reach[p, own:] = chances[p, own:] * policy[it, p, rows + own : rows + span]
        for b in range(near):
            seen = slice(b * rows, (b + 1) * rows)
            kept = slice((b + 1) * rows, (b + 2) * rows)
            open_hands = free[b : b + 1, :]
            facing = jnp.concatenate([reach[p, seen] for p in range(2)], axis=0)
            facing = facing * open_hands[:, :hands]
            coarse = facing.astype(BF16).astype(F32)
            split[b, :, :hands] = jnp.concatenate([coarse, facing - coarse], axis=0).astype(BF16)
            summed = jnp.concatenate([
                jnp.dot(
                    split[b],
                    jnp.concatenate([payoff[b, k].reshape(width, LANES) for k in range(c, min(c + 2, blocks))], axis=1),
                    preferred_element_type=F32)
                for c in range(0, blocks, 2)], axis=1)
            stake = jnp.concatenate([pots[seen, :1]] * 2, axis=0)
            summed = (summed[: 2 * rows] + summed[2 * rows :])[:, :hands] + facing
            summed = summed * open_hands[:, :hands] * stake
            values[it, 1, kept] = summed[:rows]
            values[it, 0, kept] = summed[rows:]
            if b == 0 and it < last:
                @pl.when(spot > 0)
                def _(it=it):
                    push(
                        values.at[it, :, pl.ds(rows + edge, rows - edge)], landed.at[:, pl.ds(edge, rows - edge)],
                        device_at(spot - 1), PUT_LOW, GET_HIGH)

            if b == half - 1 and it < last:
                @pl.when(spot < hub)
                def _(it=it):
                    push(
                        values.at[it, :, pl.ds(rows + own - edge, edge)], values.at[it, :, pl.ds(rows - edge, edge)],
                        device_at(spot + 1), PUT_HIGH, GET_LOW)

                @pl.when(spot > 0)
                def _(it=it):
                    push(
                        values.at[it, :, pl.ds(2 * rows, rest)], landed.at[:, pl.ds(rows, rest)],
                        device_at(spot - 1), PUT_LOWER, GET_HIGHER)
            if b == half - 1 and it == last:
                push(
                    values.at[it, other, pl.ds(rows, own)],
                    last_values.at[pl.ds(pl.multiple_of(rows + player * own, rows), own)], partner, PUT_VALUES, GET_VALUES)

                @pl.when((player == 1) & (me < n - 1))
                def _(it=it):
                    for p in range(2):
                        push(
                            values.at[it, p, pl.ds(rows + own - edge, edge)], last_values.at[pl.ds(rows - edge, edge)],
                            {"leaf": me + 1, "player": p}, PUT_EDGE + p, GET_EDGE_LOW)

                @pl.when((player == 0) & (me > 0))
                def _(it=it):
                    for p in range(2):
                        push(
                            values.at[it, p, pl.ds(rows, edge)], last_values.at[pl.ds(rows + local, edge)],
                            {"leaf": me - 1, "player": p}, PUT_EDGE + p, GET_EDGE_HIGH)

        gained = jnp.concatenate([values[it, p, rows : rows + span] for p in range(2)], axis=0)
        played = jnp.concatenate([policy[it, p, rows : rows + span] for p in range(2)], axis=0)
        instant = (gained - node_totals(same_own[...], played * gained)) * weight[:, :1]
        squares = jnp.sum((instant * instant).reshape(2, span, hands), axis=1)
        square_out[it] = jnp.broadcast_to(jnp.sum(squares, axis=1, keepdims=True), (2, LANES))

        if it == 0:
            @pl.when(spot < hub)
            def _():
                pl.semaphore_wait(all_in, 1)

        def tell(t, carry, it=it):
            at = t if it == last else jnp.where(spot < n, 2 * n - 2 - t, t)
            ahead = (at >= spot).astype(jnp.int32)
            pltpu.make_async_remote_copy(
                src_ref=square_out.at[it], dst_ref=square_in.at[it, spot - 1 + ahead],
                send_sem=square_send.at[it], recv_sem=square_recv.at[it],
                device_id=at + ahead, device_id_type=pl.DeviceIdType.LOGICAL).start()
            return carry

        lax.fori_loop(0, 2 * n - 1, tell, 0)

        if it == last:
            standing_one[...] = standing.reshape(2, total, hands)
            push(
                policy.at[it, other, pl.ds(pl.multiple_of(player * rows, rows), span)],
                last_policy.at[pl.ds(pl.multiple_of(player * span, rows), span)], partner, PUT_POLICY, GET_POLICY)
            push(
                standing_one.at[other, pl.ds(rows, own)], last_regrets.at[pl.ds(pl.multiple_of(player * own, rows), own)],
                partner, PUT_REGRETS, GET_REGRETS)

        if it == 0:
            same_last[...] = same_of(ids_of(player, me * local - rows, local + 2 * rows))
            @pl.when((player == 0) & (me > 0))
            def _():
                for p in range(2):
                    settle(late_before.at[p, pl.ds(rows - edge, edge)], get.at[GET_LATE + p])

            @pl.when((player == 1) & (me < n - 1))
            def _():
                for p in range(2):
                    settle(late_after.at[p, pl.ds(edge, rows - edge)], get.at[GET_AFTER + p])
                    settle(late_after.at[p, pl.ds(rows, rest)], get.at[GET_BEYOND + p])

            standing = jnp.concatenate([
                part for p in range(2) for part in (
                    held[p, :rows] + late_before[p], held[p, rows : rows + own],
                    held[p, rows + own :] + late_after[p])], axis=0)
            policy[0] = strategy(standing).reshape(2, total, hands)
            for p in range(2):
                beside = slice(p * total + rows + own, p * total + rows + span)
                forth = ids[p][rows + own : rows + span] == ids[p][rows + own - 1 : rows + own]
                factor = jnp.where(forth, jnp.maximum(standing[beside], 0.0) + DELTA, policy[0, p, rows + own : rows + span])
                chances[p, own:] = jnp.where(player == 0, chances[p, own:], ahead[p] / factor)

        if it < last:
            @pl.when(spot > 0)
            def _(it=it):
                settle(values.at[it, :, pl.ds(rows - edge, edge)], get.at[GET_LOW])

            @pl.when(spot < hub)
            def _():
                settle(landed.at[:, pl.ds(edge, rows - edge)], get.at[GET_HIGH])
                settle(landed.at[:, pl.ds(rows, rest)], get.at[GET_HIGHER])

            inner = lax.broadcasted_iota(jnp.int32, (rows, hands), 0) < edge
            gained = jnp.concatenate([
                part for p in range(2) for part in (
                    values[it, p, : rows + own], jnp.where(inner, values[it, p, rows + own : rows + span], landed[p, :rows]),
                    landed[p, rows:])], axis=0)
            instant = gained - node_totals(same[...], policy[it].reshape(2 * total, hands) * gained)
        else:
            mine = pl.ds(pl.multiple_of(player * span, rows), span)
            last_policy[mine] = policy[it, player, pl.ds(pl.multiple_of(player * rows, rows), span)]
            last_regrets[pl.ds(pl.multiple_of(player * own, rows), own)] = standing_one[player, pl.ds(rows, own)]
            last_values[pl.ds(pl.multiple_of(rows + player * own, rows), own)] = values[it, player, pl.ds(rows, own)]
            settle(last_policy.at[pl.ds(pl.multiple_of(other * span, rows), span)], get.at[GET_POLICY])
            settle(last_regrets.at[pl.ds(pl.multiple_of(other * own, rows), own)], get.at[GET_REGRETS])
            settle(last_values.at[pl.ds(pl.multiple_of(rows + other * own, rows), own)], get.at[GET_VALUES])

            @pl.when(me > 0)
            def _():
                settle(last_values.at[pl.ds(rows - edge, edge)], get.at[GET_EDGE_LOW])

            @pl.when(me < n - 1)
            def _():
                settle(last_values.at[pl.ds(rows + local, edge)], get.at[GET_EDGE_HIGH])

            gained = last_values[...]
            instant = (gained - node_totals(same_last[...], last_policy[...] * gained))[rows : rows + local]
            outs[1] = gained[rows : rows + local]

        everyone = square_in.at[it]
        settle(everyone, square_recv.at[it])

        squares = square_out[it] + jnp.sum(square_in[it], axis=0)
        inverse = 1.0 / jnp.sqrt(squares / (leaf_count * hands) + EPSILON)
        if it < last:
            turn = lax.broadcasted_iota(jnp.int32, (2 * total, 1), 0) < total
            standing = standing + instant * jnp.where(turn, inverse[0:1, :1], inverse[1:2, :1])
        else:
            outs[0] = last_regrets[...] + instant * jnp.where(player == 0, inverse[0:1, :1], inverse[1:2, :1])

    def sent(view, slot):
        settle(view, put.at[slot])

    @pl.when(me > 0)
    def _():
        @pl.when(player == 1)
        def _():
            sent(info, PUT_INFO)

        sent(regrets.at[0, pl.ds(0, edge)], PUT_NEXT)
        sent(ahead_out.at[pl.ds(0, edge)], PUT_AHEAD)
        sent(regrets.at[0, pl.ds(edge, rows - edge)], PUT_AFTER)
        sent(regrets.at[0, pl.ds(rows, rest)], PUT_BEYOND)

    @pl.when(me < n - 1)
    def _():
        sent(behind_out, PUT_BEHIND)
        sent(regrets.at[0, pl.ds(local - edge, edge)], PUT_LATE)

    sent(parents.at[player], PUT_PARENT)

    @pl.when(player == 0)
    def _():
        sent(regrets.at[0, pl.ds(own - rows, own + rows)], PUT_HALF)
        sent(chance.at[0, pl.ds(own, own)], PUT_CHANCE)

    @pl.when(player == 1)
    def _():
        sent(regrets.at[0, pl.ds(0, own + 2 * rows)], PUT_HALF)
        sent(chance.at[0, pl.ds(0, span)], PUT_CHANCE)

    for it in range(last):
        @pl.when(spot < hub)
        def _(it=it):
            sent(values.at[it, :, pl.ds(rows + own - edge, edge)], PUT_HIGH)

        @pl.when(spot > 0)
        def _(it=it):
            sent(values.at[it, :, pl.ds(rows + edge, rows - edge)], PUT_LOW)
            sent(values.at[it, :, pl.ds(2 * rows, rest)], PUT_LOWER)

    sent(policy.at[last, other, pl.ds(pl.multiple_of(player * rows, rows), span)], PUT_POLICY)
    sent(standing_one.at[other, pl.ds(rows, own)], PUT_REGRETS)
    sent(values.at[last, other, pl.ds(rows, own)], PUT_VALUES)

    @pl.when((player == 1) & (me < n - 1))
    def _():
        for p in range(2):
            sent(values.at[last, p, pl.ds(rows + own - edge, edge)], PUT_EDGE + p)

    @pl.when((player == 0) & (me > 0))
    def _():
        for p in range(2):
            sent(values.at[last, p, pl.ds(rows, edge)], PUT_EDGE + p)

    for it in range(ITERS):
        everyone = square_in.at[it]
        settle(everyone, square_send.at[it])


def kernel(n, boards, rows, hands, leaf_count, *refs):
    near = boards // 2 + 1
    span = near * rows
    total = span + 2 * rows
    edged = (boards + 2) * rows
    width = round_up(hands, LANES)
    depth = round_up(DECK_SIZE + 1, 32)
    pl.run_scoped(
        functools.partial(body, n, boards, rows, hands, leaf_count, *refs),
        pltpu.VMEM((near, width // LANES, PARTS, width // PARTS, LANES), F8),
        pltpu.VMEM((width // LANES, PARTS, width // PARTS, LANES), BF16),
        pltpu.VMEM((width, depth), F8),
        pltpu.VMEM((near, PARTS, width // PARTS, LANES), BF16),
        pltpu.VMEM((depth, width), F8),
        pltpu.VMEM((2 * total, 4 * total), BF16),
        pltpu.VMEM((2 * span, 4 * span), BF16),
        pltpu.VMEM((edged, 2 * edged), BF16),
        pltpu.VMEM((near, 4 * rows, width), BF16),
    )


def solution(mesh):
    n = mesh.shape["leaf"]

    def local(chance_reach, regrets_start, pot, parent, hand_cards, board_cards, hand_rank):
        leaf_rows, hands = chance_reach.shape[1:]
        boards = hand_rank.shape[0]
        rows = leaf_rows // boards
        leaf_count = parent.shape[1]
        width = round_up(hands, LANES)
        half = boards // 2
        near = half + 1
        span = near * rows
        total = (half + 3) * rows
        edged = leaf_rows + 2 * rows
        vmem = pl.BlockSpec(memory_space=pltpu.VMEM)
        shape = pltpu.VMEM(chance_reach.shape, F32)
        dma = pltpu.SemaphoreType.DMA
        arrays = (chance_reach, regrets_start, pot[None], parent, hand_cards.T, board_cards, hand_rank)
        outs = pl.pallas_call(
            functools.partial(kernel, n, boards, rows, hands, leaf_count),
            out_shape=pltpu.VMEM((2, leaf_rows, hands), F32),
            in_specs=[pl.BlockSpec(memory_space=pl.ANY)] * len(arrays),
            out_specs=vmem,
            scratch_shapes=[
                pltpu.VMEM(chance_reach.shape, F32),
                pltpu.VMEM(regrets_start.shape, F32),
                pltpu.VMEM((1, leaf_rows), F32),
                pltpu.VMEM((2, 1, leaf_count), jnp.int32),
                pltpu.VMEM((2, hands), jnp.int32),
                pltpu.VMEM(board_cards.shape, jnp.int32),
                pltpu.VMEM(hand_rank.shape, jnp.int32),
                dma((len(arrays),)),
                pltpu.VMEM((round_up(near, 8), width), F32),
                pltpu.VMEM((near, width), F32),
                pltpu.VMEM((2, width), jnp.int32),
                pltpu.VMEM((round_up(boards, 8), width), jnp.int32),
                pltpu.VMEM((1, 2 * width + LANES), F32),
                pltpu.VMEM((1, 2 * width + LANES), F32),
                pltpu.VMEM((span, LANES), F32),
                pltpu.VMEM((2 * span, LANES), F32),
                pltpu.VMEM((2, total, hands), F32),
                pltpu.VMEM((2, span, hands), F32),
                pltpu.VMEM((ITERS, 2, total, hands), F32),
                pltpu.VMEM((ITERS, 2, total, hands), F32),
                pltpu.VMEM((2, 2 * rows, hands), F32),
                pltpu.VMEM((2, total, hands), F32),
                pltpu.VMEM((ITERS, 2, LANES), F32),
                pltpu.VMEM((ITERS, 2 * n - 1, 2, LANES), F32),
                pltpu.VMEM((edged, hands), F32),
                pltpu.VMEM((leaf_rows, hands), F32),
                pltpu.VMEM((edged, hands), F32),
                pltpu.VMEM((2, span, hands), F32),
                pltpu.VMEM((2, 1, hands), F32),
                pltpu.VMEM((1, hands), F32),
                pltpu.VMEM((2, rows, hands), F32),
                pltpu.VMEM((rows, hands), F32),
                pltpu.VMEM((2, rows, hands), F32),
                pltpu.VMEM((2, 2 * rows, hands), F32),
                pltpu.SemaphoreType.REGULAR,
                dma((PUTS,)), dma((GETS,)),
                dma((ITERS,)), dma((ITERS,)),
            ],
            compiler_params=pltpu.CompilerParams(collective_id=0, has_side_effects=True),
            name="regret",
        )(*arrays)
        return outs[:1], outs[1:]

    in_specs = (
        P("player", "leaf", None),
        P("player", "leaf", None),
        P("leaf"),
        P("player", None),
        P(),
        P("leaf", None),
        P("leaf", None),
    )
    out_specs = (P("player", "leaf", None), P("player", "leaf", None))
    return jax.shard_map(local, mesh=mesh, in_specs=in_specs, out_specs=out_specs, check_vma=False)
```
